32 devices in a mesh: lon: 8 (over y, x, core), lat: 4 (over z).
Axes of the slice: x: 2, y: 2, z: 4, core: 2. Of those that a mesh axis runs over, the one named last changes fastest.
Arguments:
- height_old: float32 [1024, 512], P('lon', 'lat'), may hold values from -6 to 6
- height_now: float32 [1024, 512], P('lon', 'lat'), may hold values from -6 to 6
- zonal_old: float32 [1024, 512], P('lon', 'lat'), may hold values from -6 to 6
- zonal_now: float32 [1024, 512], P('lon', 'lat'), may hold values from -6 to 6
- meridional_old: float32 [1024, 512], P('lon', 'lat'), may hold values from -6 to 6
- meridional_now: float32 [1024, 512], P('lon', 'lat'), may hold values from -6 to 6
- ocean_depth: float32 [1024, 512], P('lon', 'lat'), may hold values from 0.2 to 1
- land_sea: int32 [1024, 512], P('lon', 'lat'), may hold values 0 or 1
- metric_factor: float32 [512], P('lat'), may hold values from 0.5 to 2
- coriolis: float32 [512], P('lat'), may hold values from -0.5 to 0.5
- implicit_weight: float32 [512], replicated, may hold values from 150 to 40000
- source_longitude: int32 [512], replicated, may hold values from 0 to 1023
- source_latitude: int32 [512], replicated, may hold values from 0 to 511
- source_amplitude: float32 [512], replicated, may hold values from -24 to 24
Outputs:
- height_final: float32 [1024, 512], P('lon', 'lat')
- zonal_final: float32 [1024, 512], P('lon', 'lat')
- meridional_final: float32 [1024, 512], P('lon', 'lat')
The draws below stay inside these ranges and needn't reach their ends.
Inputs may be any that keep to these rules, and one draw needn't show every extreme that they name: `source_longitude`: cells may repeat.
All inputs are finite; a program needn't handle non-finite values. No bound on the sum of `land_sea` on one device may be relied on, other than what follows from the above.
Results may differ from the reference program's by a relative error of at most 0.0003.
Values sent between devices are 32-bit elements; how exact they have to be, the bound alone decides.
A program may use at most 64 MiB of HBM per device.

```python
import math
import jax
import jax.numpy as jnp
from jax import lax

STEPS = 1
SOURCES = 512
NLON = 1024
NLAT = 512


def draw_implicit_weight(key, part):
    phase_key, rough_key = jax.random.split(jax.random.fold_in(key, 211))
    north = jnp.arange(NLAT, dtype=jnp.float32) / NLAT
    phase = jax.random.uniform(phase_key, (), jnp.float32, 0.0, 2.0 * math.pi)
    wave = 0.5 + 0.5 * jnp.cos(4.0 * math.pi * north + phase)
    rough = jax.random.uniform(rough_key, (NLAT,), jnp.float32, 0.5, 1.0)
    level = 2.5 + 2.0 * wave
    return jnp.power(10.0, level).astype(jnp.float32) * rough


def draw_height_old(key, part):
    rough_key = jax.random.fold_in(jax.random.fold_in(key, 101), 0)
    return jax.random.truncated_normal(rough_key, -6.0, 6.0, (NLON, NLAT), jnp.float32)


def with_ends(array, own_key, least, largest):
    longest = array.shape.index(max(array.shape))
    spots = []
    for shift in (0, 1):
        where = [jax.random.randint(jax.random.fold_in(own_key, axis), (), 0, length) for axis, length in enumerate(array.shape)]
        where[longest] = (where[longest] + shift) % array.shape[longest]
        spots.append(tuple(where))
    return array.at[spots[0]].set(least).at[spots[1]].set(largest)


def levels(key, shape, cuts, least, largest):
    factor_of, own = 1.0, jax.random.fold_in(key, 6)
    for dim, blocks in cuts:
        steps = jnp.exp(jax.random.uniform(jax.random.fold_in(own, dim), (blocks,), jnp.float32, least / len(cuts), largest / len(cuts)))
        factor_of = factor_of * jnp.repeat(steps, shape[dim] // blocks).reshape([-1 if axis == dim else 1 for axis in range(len(shape))])
    return factor_of


def scatter_about(key, dims, spread, limit, cuts=(), held_as=jnp.bfloat16):
    drawn = jax.random.normal(key, dims, jnp.float32) * spread
    if len(cuts) > 0:
        drawn = levels(key, dims, cuts, -0.22, 0.18) * drawn
    return jnp.clip(drawn, min=-limit, max=limit).astype(held_as)


def setup_inputs(seed: int = 0) -> dict:
    arg_keys = jax.random.split(jax.random.key(seed), 15)
    return {
        "height_old": draw_height_old(jax.random.fold_in(arg_keys[14], 71), 0),
        "height_now": scatter_about(arg_keys[1], (NLON, NLAT), 1.0, 6.0, ((0, 8), (1, 4)), jnp.float32),
        "zonal_old": scatter_about(arg_keys[2], (NLON, NLAT), 1.0, 6.0, ((0, 8), (1, 4)), jnp.float32),
        "zonal_now": scatter_about(arg_keys[3], (NLON, NLAT), 1.0, 6.0, ((0, 8), (1, 4)), jnp.float32),
        "meridional_old": scatter_about(arg_keys[4], (NLON, NLAT), 1.0, 6.0, ((0, 8), (1, 4)), jnp.float32),
        "meridional_now": scatter_about(arg_keys[5], (NLON, NLAT), 1.0, 6.0, ((0, 8), (1, 4)), jnp.float32),
        "ocean_depth": jnp.clip(jnp.exp(math.log(1.0) - 1.609438 * jax.random.uniform(arg_keys[6], (NLON, NLAT), jnp.float32) ** levels(arg_keys[6], (NLON, NLAT), ((0, 8), (1, 4)), -0.2, 0.2)), 0.2, 1.0),
        "land_sea": with_ends((jax.random.randint(arg_keys[7], (NLON, NLAT), 0, 5) < 4).astype(jnp.int32), jax.random.fold_in(arg_keys[7], 1), 0, 1),
        "metric_factor": jnp.clip(jnp.exp(math.log(2.0) - 1.3862944 * jax.random.uniform(arg_keys[8], (NLAT,), jnp.float32) ** levels(arg_keys[8], (NLAT,), ((0, 4),), -0.2, 0.2)), 0.5, 2.0),
        "coriolis": jnp.clip(jax.random.uniform(arg_keys[9], (NLAT,), jnp.float32, -0.5, 0.5) * levels(arg_keys[9], (NLAT,), ((0, 4),), -0.4, 0.0), -0.5, 0.5),
        "implicit_weight": draw_implicit_weight(jax.random.fold_in(arg_keys[14], 71), 0),
        "source_longitude": with_ends(jax.random.randint(arg_keys[11], (SOURCES,), 0, NLON), jax.random.fold_in(arg_keys[11], 1), 0, NLON - 1).astype(jnp.int32),
        "source_latitude": with_ends(jax.random.randint(arg_keys[12], (SOURCES,), 0, NLAT), jax.random.fold_in(arg_keys[12], 1), 0, NLAT - 1).astype(jnp.int32),
        "source_amplitude": scatter_about(arg_keys[13], (SOURCES,), 4.0, 24.0, (), jnp.float32),
    }


COURANT = 0.25

def line_solve(rhs, weight):
    length = weight.shape[0]
    position = jnp.arange(length)
    lower = jnp.where(position > 0, -weight, jnp.zeros_like(weight))
    upper = jnp.where(position < length - 1, -weight, jnp.zeros_like(weight))
    middle = 1.0 + 2.0 * weight
    shape = rhs.shape
    solved = lax.linalg.tridiagonal_solve(jnp.broadcast_to(lower, shape), jnp.broadcast_to(middle, shape), jnp.broadcast_to(upper, shape), rhs[..., None])
    return solved[..., 0]

def east_diff(field):
    return jnp.roll(field, -1, 0) - jnp.roll(field, 1, 0)

def north_diff(field):
    upper = jnp.pad(field[:, 1:], ((0, 0), (0, 1)))
    lower = jnp.pad(field[:, :-1], ((0, 0), (1, 0)))
    return upper - lower

def reference(height_old, height_now, zonal_old, zonal_now, meridional_old, meridional_now, ocean_depth, land_sea, metric_factor, coriolis, implicit_weight, source_longitude, source_latitude, source_amplitude):
    wetness = land_sea.astype(height_old.dtype)
    metric = metric_factor[None, :]
    turning = coriolis[None, :]
    for _ in range(STEPS):
        flux_east = ocean_depth * wetness * zonal_now
        flux_north = ocean_depth * wetness * meridional_now
        interim = height_old - COURANT * (metric * east_diff(flux_east) + north_diff(flux_north))
        interim = interim.at[source_longitude, source_latitude].add(source_amplitude)
        zonal_next = wetness * (zonal_old - COURANT * metric * east_diff(height_now) + turning * meridional_now)
        meridional_next = wetness * (meridional_old - COURANT * north_diff(height_now) - turning * zonal_now)
        height_next = wetness * line_solve(interim, implicit_weight)
        height_old, zonal_old, meridional_old = (height_now, zonal_now, meridional_now)
        height_now, zonal_now, meridional_now = (height_next, zonal_next, meridional_next)
    return (height_now, zonal_now, meridional_now)
```

```python
import functools

import jax
import jax.numpy as jnp
from jax import lax
from jax.experimental import pallas as pl
from jax.experimental.pallas import tpu as pltpu
from jax.sharding import PartitionSpec as P

COURANT = 0.25
MESH = pl.DeviceIdType.MESH
HIGHEST = lax.Precision.HIGHEST
LAST_WITH_LAST = (((1,), (1,)), ((), ()))
FIRST_WITH_FIRST = (((0,), (0,)), ((), ()))
PLAIN = (((1,), (0,)), ((), ()))
WINDOW = 16
STRIDES = 8


def exact_dot(left, right, dims):
    return lax.dot_general(left, right, dims, precision=HIGHEST, preferred_element_type=jnp.float32)


def pieces(value):
    found = []
    for _ in range(3):
        piece = value.astype(jnp.bfloat16).astype(jnp.float32)
        found.append(piece)
        value = value - piece
    return found


def line_scan(a, lane, upward):
    rows = a.shape[1]
    one, zero = jnp.ones_like(a), jnp.zeros_like(a)

    def behind(v, amount):
        return pltpu.roll(v, amount if upward else rows - amount, 1)

    def inside(amount):
        return lane >= amount if upward else lane < rows - amount

    window = min(WINDOW, rows)
    m = [one, zero, zero, one]
    for i in range(window - 1, -1, -1):
        step = behind(a, i) if i else a
        keep = inside(i)
        for x, y in ((0, 2), (1, 3)):
            total = m[x] + m[y]
            grown = m[x] + step * total
            m[x] = jnp.where(keep, grown, m[x]) if i else grown
            m[y] = jnp.where(keep, total, m[y]) if i else total
    unit = (1.0, 0.0, 0.0, 1.0)
    while window < rows:
        count = min(STRIDES, rows // window)
        terms = [m]
        for i in range(1, count):
            keep = inside(i * window)
            terms.append([jnp.where(keep, behind(v, i * window), u) for v, u in zip(m, unit)])
        while len(terms) > 1:
            joined = []
            for p, q in zip(terms[0::2], terms[1::2]):
                joined.append(
                    [
                        p[0] * q[0] + p[1] * q[2],
                        p[0] * q[1] + p[1] * q[3],
                        p[2] * q[0] + p[3] * q[2],
                        p[2] * q[1] + p[3] * q[3],
                    ]
                )
            terms = joined + terms[2 * len(joined) :]
        m = terms[0]
        window *= count
    return m


def line_factors(a, up, down, before, after, blocks):
    padded, rows = a.shape
    one = jnp.ones_like(a)

    def carried(m, edge, order):
        m = [jnp.broadcast_to(v[:, edge : edge + 1], (padded, rows)) for v in m]
        x, y = one[:1], jnp.zeros_like(one[:1])
        xs, ys, shrink = {}, {}, {}
        for c in order:
            xs[c], ys[c] = x, y
            nx = m[0][c : c + 1] * x + m[1][c : c + 1] * y
            ny = m[2][c : c + 1] * x + m[3][c : c + 1] * y
            ratio = 1.0 / (nx + ny)
            shrink[c] = ratio
            x, y = nx * ratio, ny * ratio
        spare = [one[:1]] * (padded - blocks)
        return [jnp.concatenate([t[c] for c in range(blocks)] + spare, axis=0) for t in (xs, ys, shrink)]

    x_in, y_in, shrink_up = carried(up, rows - 1, range(blocks))
    xb_in, yb_in, shrink_down = carried(down, 0, range(blocks - 1, -1, -1))
    x = up[0] * x_in + up[1] * y_in
    y = up[2] * x_in + up[3] * y_in
    yb = down[2] * xb_in + down[3] * yb_in
    end = lambda v: jnp.broadcast_to(v[:, rows - 1 :], (padded, rows))
    scale = 1.0 / (end(x) + end(y) * xb_in)
    return (
        a * y,
        a * yb,
        y * scale,
        yb * scale,
        shrink_up,
        shrink_down,
        x_in,
        y_in,
        xb_in,
        yb_in,
        -before * y_in,
        after * yb_in,
    )


def kernel(lons, lats, *refs):
    ins, outs, refs = refs[:14], refs[14:17], refs[17:]
    (
        fields,
        land,
        pair,
        wgt,
        slon,
        slat,
        amp,
        load_sem,
        factors,
        starts,
        send_lat,
        send_side,
        send_next,
        recv_lat,
        recv_side,
        recv_next,
        send_sem,
        recv_sem,
    ) = refs
    a_id = lax.axis_index("lon")
    b_id = lax.axis_index("lat")
    sides = (lax.rem(a_id + lons - 1, lons), lax.rem(a_id + 1, lons))
    znow, depth, hnow, mnow, hold, zold, mold = (fields.at[k] for k in range(7))
    met, cor, samp = pair.at[0], pair.at[1], amp.at[0]
    columns, rows = land.shape
    padded = wgt.shape[0]

    barrier = pltpu.get_barrier_semaphore()
    for group, number, to in (
        (0, 3, znow),
        (0, 6, depth),
        (0, 7, land),
        (0, 1, hnow),
        (1, 8, met),
        (1, 9, cor),
        (2, 10, wgt.at[pl.ds(0, lats)]),
        (3, 5, mnow),
        (3, 0, hold),
        (4, 11, slon),
        (4, 12, slat),
        (4, 13, samp),
        (3, 2, zold),
        (3, 4, mold),
    ):
        pltpu.make_async_copy(ins[number], to, load_sem.at[group]).start()

    def loaded(group, ref):
        pltpu.make_async_copy(ref, ref, load_sem.at[group]).wait()

    for k in range(1, lats):
        other = lax.rem(b_id + k, lats)
        for column in (*sides, a_id):
            pl.semaphore_signal(barrier, inc=1, device_id=(column, other), device_id_type=MESH)
    for side in sides:
        pl.semaphore_signal(barrier, inc=1, device_id=(side, b_id), device_id_type=MESH)

    loaded(0, fields.at[pl.ds(0, 4)])
    loaded(1, pair)
    scaled_metric = COURANT * met[...]
    for side, (at, sign) in enumerate(((0, -1.0), (columns - 1, 1.0))):
        edge = pl.ds(at, 1)
        flux = depth[edge, :] * land[edge, :].astype(jnp.float32) * znow[edge, :]
        flux = sign * scaled_metric * flux
        send_side[side] = flux
        send_next[side] = jnp.concatenate([flux, hnow[edge, :]], axis=0)

    def remote(src, dst, kind, column, row):
        return pltpu.make_async_remote_copy(
            src_ref=src,
            dst_ref=dst,
            send_sem=send_sem.at[kind],
            recv_sem=recv_sem.at[kind],
            device_id=(column, row),
            device_id_type=MESH,
        )

    def greet_and_send_edges():
        pl.semaphore_wait(barrier, 3 * lats - 1)
        for k in range(1, lats):
            for side in (1, 0):
                remote(
                    send_side.at[side],
                    recv_side.at[side, lats - k - 1],
                    0,
                    sides[side],
                    lax.rem(b_id + k, lats),
                ).start()
        for side in (0, 1):
            remote(send_next.at[side], recv_next.at[side], 1, sides[side], b_id).start()

    far = jnp.logical_and(b_id == lats - 1, a_id > 1)
    pl.when(far)(greet_and_send_edges)

    loaded(2, wgt.at[pl.ds(0, lats)])
    weight = wgt[...]
    if padded > lats:
        row_id = lax.broadcasted_iota(jnp.int32, (padded, rows), 0)
        weight = jnp.where(row_id < lats, weight, 1.0)
    a = 1.0 / weight
    lane_of = lax.broadcasted_iota(jnp.int32, (padded, rows), 1)
    first_lane, last_lane = lane_of == 0, lane_of == rows - 1
    before = COURANT * pltpu.roll(jnp.broadcast_to(a[:, rows - 1 :], (padded, rows)), 1, 0)
    after = COURANT * pltpu.roll(jnp.broadcast_to(a[:, :1], (padded, rows)), padded - 1, 0)
    up = line_scan(a, lane_of, True)
    down = line_scan(a, lane_of, False)
    zeros = jnp.zeros_like(a)
    at_last = lambda v: jnp.where(last_lane, v, zeros)
    at_first = lambda v: jnp.where(first_lane, v, zeros)
    for k, value in enumerate(
        (
            a * up[2],
            a * up[3],
            a * down[2],
            a * down[3],
            at_last((up[0] + up[2]) * after),
            at_last((up[1] + up[3]) * after) - at_first(before),
            -at_first((down[0] + down[2]) * before),
            at_last(after) - at_first((down[1] + down[3]) * before),
        )
    ):
        starts[k] = value

    loaded(3, fields.at[pl.ds(3, 4)])
    loaded(4, amp)
    wet = land[...].astype(jnp.float32)
    wet_depth = depth[...] * wet
    flux_east = wet_depth * znow[...]
    flux_north = wet_depth * mnow[...]
    metric = met[...]
    line = lax.broadcasted_iota(jnp.int32, (columns, rows), 0)
    lane = lax.broadcasted_iota(jnp.int32, (columns, rows), 1)

    def inner_diff(v, axis, position, size):
        ahead = jnp.where(position == size - 1, 0.0, pltpu.roll(v, size - 1, axis))
        behind = jnp.where(position == 0, 0.0, pltpu.roll(v, 1, axis))
        return ahead - behind

    rhs = hold[...] - COURANT * (
        metric * inner_diff(flux_east, 0, line, columns) + inner_diff(flux_north, 1, lane, rows)
    )
    sources = slon.shape[1]
    east_cell = lax.broadcasted_iota(jnp.int32, (columns, sources), 0) + a_id * columns
    north_cell = lax.broadcasted_iota(jnp.int32, (rows, sources), 0) + b_id * rows
    hit_east = jnp.where(east_cell == slon[...], 1.0, 0.0).astype(jnp.bfloat16)
    hit_north = north_cell == slat[...]
    for piece in pieces(samp[...]):
        rhs = rhs + lax.dot_general(
            hit_east,
            jnp.where(hit_north, piece, 0.0).astype(jnp.bfloat16),
            LAST_WITH_LAST,
            preferred_element_type=jnp.float32,
        )

    height = hnow[...]
    row_lane = lax.broadcasted_iota(jnp.int32, (1, rows), 1)
    first_row = jnp.where(row_lane == 0, 1.0, 0.0)
    last_row = jnp.where(row_lane == rows - 1, 1.0, 0.0)
    zero_row = jnp.zeros((1, rows), jnp.float32)
    outer = exact_dot(
        jnp.concatenate([zero_row, zero_row, last_row, zero_row] + [zero_row] * 2 + [first_row, zero_row], axis=0),
        height,
        LAST_WITH_LAST,
    )
    ends = exact_dot(
        jnp.concatenate([first_row, last_row] + [zero_row] * 6, axis=0), flux_north, LAST_WITH_LAST
    )

    def start(k):
        return starts[k, pl.ds(b_id, 1), :]

    def laid(k):
        return jnp.concatenate(
            [start(k), start(k + 1), zero_row, zero_row, start(k + 2), start(k + 3), zero_row, zero_row], axis=0
        )

    moments = outer + exact_dot(
        jnp.concatenate([laid(0), laid(4)], axis=1),
        jnp.concatenate([rhs, flux_north], axis=1),
        LAST_WITH_LAST,
    )
    send_lat[0] = moments[0:4]
    send_lat[1] = moments[4:8]
    pl.when(jnp.logical_not(far))(greet_and_send_edges)
    for k in range(1, lats):
        remote(
            send_lat.at[jnp.where(b_id + k < lats, 0, 1)],
            recv_lat.at[lats - k - 1],
            2,
            a_id,
            lax.rem(b_id + k, lats),
        ).start()

    for k, value in enumerate(line_factors(a, up, down, before, after, lats)):
        factors[k] = value

    def own(k, block):
        return factors[k, pl.ds(block, 1), :]

    ay, ayb, y_s, yb_s = [own(k, b_id) for k in range(4)]
    columns_of = jnp.transpose(jnp.concatenate([ay, ayb] + [zero_row] * 6, axis=0))
    source_lat = lax.broadcasted_iota(jnp.int32, (rows, rows), 0)
    target_lat = lax.broadcasted_iota(jnp.int32, (rows, rows), 1)
    below = source_lat <= target_lat
    inverse = jnp.where(below, columns_of[:, 0:1] * yb_s, columns_of[:, 1:2] * y_s)
    outs[0][...] = exact_dot(rhs, inverse, PLAIN)
    turning = cor[...]
    outs[1][...] = wet * (
        zold[...] + turning * mnow[...] - COURANT * metric * inner_diff(height, 0, line, columns)
    )
    outs[2][...] = mold[...] - COURANT * inner_diff(height, 1, lane, rows) - turning * znow[...]

    def across(v):
        return v[:, :columns] if columns <= rows else jnp.broadcast_to(v[:, :1], (1, columns))

    coarse, fine, reach = [None] * lats, [None] * lats, [None] * lats
    product = jnp.ones((1, rows), jnp.float32)
    for d in range(lats - 1, 0, -1):
        block = lax.rem(b_id + d, lats)
        product = product * own(4, block)
        coarse[d], fine[d], reach[d] = own(6, block) * product, own(7, block) * product, own(0, block) * product
    product = jnp.ones((1, rows), jnp.float32)
    for d in range(1, lats):
        block = lax.rem(b_id + d, lats)
        north = b_id + d < lats
        product = product * own(5, block)
        coarse[d] = jnp.where(north, own(8, block) * product, coarse[d])
        fine[d] = jnp.where(north, own(9, block) * product, fine[d])
        reach[d] = jnp.where(north, own(1, block) * product, reach[d])
    own_low = across(own(10, b_id)) * ends[0:1]
    own_high = across(own(11, b_id)) * ends[1:2]
    basis = pieces(
        jnp.concatenate(
            [
                jnp.concatenate([yb_s, y_s] + [zero_row] * 6, axis=0),
                jnp.concatenate([zero_row, zero_row, COURANT * first_row, -COURANT * last_row] + [zero_row] * 4, axis=0),
            ],
            axis=1,
        )
    )
    basis = jnp.concatenate([basis[k] for k in (0, 1, 2, 0, 1, 0)], axis=0).astype(jnp.bfloat16)
    full = jnp.ones((rows, rows), jnp.float32)
    lower = jnp.where(below, 1.0, 0.0)
    running = jnp.concatenate(
        [jnp.concatenate([lower, full], axis=0), jnp.concatenate([1.0 - lower, full], axis=0)], axis=1
    ).astype(jnp.bfloat16)

    arrivals = ((2, recv_lat), (1, recv_next), (0, recv_side))
    for kind, ref in arrivals:
        remote(ref, ref, kind, sides[0], b_id).wait_recv()

    low, high = own_low, own_high
    for d in range(1, lats):
        arrived = recv_lat[d - 1, 0:1] * across(coarse[d]) + recv_lat[d - 1, 1:2] * across(fine[d])
        north = b_id + d < lats
        high = high + jnp.where(north, arrived, 0.0)
        low = low + jnp.where(north, 0.0, arrived)
    south_height = jnp.where(b_id > 0, recv_lat[lats - 2, 2:3], 0.0)
    north_height = jnp.where(b_id < lats - 1, recv_lat[0, 2:3], 0.0)
    carried = pieces(
        jnp.concatenate([low, high, south_height, north_height, jnp.zeros((4, columns), jnp.float32)], axis=0)
    )
    carried = jnp.concatenate([carried[k] for k in (0, 0, 0, 1, 1, 2)], axis=0).astype(jnp.bfloat16)
    corrections = lax.dot_general(carried, basis, FIRST_WITH_FIRST, preferred_element_type=jnp.float32)

    lows, highs = [], []
    for side in (1, 0):
        flux = recv_next[side, 0:1]
        low, high = zero_row, zero_row
        for d in range(1, lats):
            arrived = recv_side[side, d - 1] * reach[d]
            north = b_id + d < lats
            high = high + jnp.where(north, arrived, 0.0)
            low = low + jnp.where(north, 0.0, arrived)
        lows.append(jnp.concatenate([flux * ay, low], axis=1))
        highs.append(jnp.concatenate([flux * ayb, high], axis=1))
    spare = jnp.zeros((4, 2 * rows), jnp.float32)
    edges = jnp.concatenate(pieces(jnp.concatenate(lows + highs + [spare], axis=0)), axis=0)
    edges = jnp.concatenate([edges, jnp.zeros((8, 2 * rows), jnp.float32)], axis=0).astype(jnp.bfloat16)
    edges = lax.dot_general(edges, running, PLAIN, preferred_element_type=jnp.float32)
    edges = edges[0:8] + edges[8:16] + edges[16:24]

    solved = outs[0][...] + corrections[:, :rows]
    outs[0][...] = wet * solved
    outs[2][...] = wet * (outs[2][...] + corrections[:, rows:])
    for k, (at, side, sign) in enumerate(((0, 1, COURANT), (columns - 1, 0, -COURANT))):
        edge = pl.ds(at, 1)
        outs[0][edge, :] = wet[at : at + 1] * (
            solved[at : at + 1] + edges[k : k + 1, :rows] * yb_s + edges[2 + k : 3 + k, rows:] * y_s
        )
        outs[1][edge, :] = outs[1][edge, :] + wet[at : at + 1] * (sign * metric * recv_next[side, 1:2])
    for kind, ref in arrivals:
        remote(ref, ref, kind, sides[0], b_id).wait_send()


def store_kernel(*refs):
    stores = [
        pltpu.make_async_copy(refs[k], refs[3 + k], refs[6].at[k]) for k in range(3)
    ]
    for store in stores:
        store.start()
    for store in stores:
        store.wait()


def per_device(lons, lats, *args):
    args = list(args)
    columns, rows = args[0].shape
    sources = args[11].shape[0]
    padded = -(-lats // 8) * 8
    args[8] = args[8].reshape(1, rows)
    args[9] = args[9].reshape(1, rows)
    args[10] = args[10].reshape(lats, rows)
    for k in (11, 12, 13):
        args[k] = args[k].reshape(1, sources)
    out = pltpu.VMEM((columns, rows), jnp.float32)
    others = lats - 1
    results = pl.pallas_call(
        functools.partial(kernel, lons, lats),
        out_shape=(out, out, out),
        in_specs=[pl.BlockSpec(memory_space=pl.ANY)] * 14,
        out_specs=(pl.BlockSpec(memory_space=pltpu.VMEM),) * 3,
        scratch_shapes=[
            pltpu.VMEM((7, columns, rows), jnp.float32),
            pltpu.VMEM((columns, rows), jnp.int32),
            pltpu.VMEM((2, 1, rows), jnp.float32),
            pltpu.VMEM((padded, rows), jnp.float32),
            pltpu.VMEM((1, sources), jnp.int32),
            pltpu.VMEM((1, sources), jnp.int32),
            pltpu.VMEM((3, 1, sources), jnp.float32),
            pltpu.SemaphoreType.DMA((5,)),
            pltpu.VMEM((12, padded, rows), jnp.float32),
            pltpu.VMEM((8, padded, rows), jnp.float32),
            pltpu.VMEM((2, 4, columns), jnp.float32),
            pltpu.VMEM((2, 1, rows), jnp.float32),
            pltpu.VMEM((2, 2, rows), jnp.float32),
            pltpu.VMEM((others, 4, columns), jnp.float32),
            pltpu.VMEM((2, others, 1, rows), jnp.float32),
            pltpu.VMEM((2, 2, rows), jnp.float32),
            pltpu.SemaphoreType.DMA((3,)),
            pltpu.SemaphoreType.DMA((3,)),
        ],
        compiler_params=pltpu.CompilerParams(collective_id=0, has_side_effects=True),
    )(*args)
    return pl.pallas_call(
        store_kernel,
        out_shape=(jax.ShapeDtypeStruct((columns, rows), jnp.float32),) * 3,
        in_specs=[pl.BlockSpec(memory_space=pltpu.VMEM)] * 3,
        out_specs=(pl.BlockSpec(memory_space=pl.ANY),) * 3,
        scratch_shapes=[pltpu.SemaphoreType.DMA((3,))],
    )(*[pltpu.with_memory_space_constraint(r, pltpu.VMEM) for r in results])


def solution(mesh):
    field = P("lon", "lat")
    placed = (field,) * 8 + (P("lat"),) * 2 + (P(),) * 4
    return jax.shard_map(
        functools.partial(per_device, mesh.shape["lon"], mesh.shape["lat"]),
        mesh=mesh,
        in_specs=placed,
        out_specs=(field,) * 3,
        check_vma=False,
    )
```

```python
import functools

import jax
import jax.numpy as jnp
from jax import lax
from jax.experimental import pallas as pl
from jax.experimental.pallas import tpu as pltpu
from jax.sharding import PartitionSpec as P

COURANT = 0.25
MESH = pl.DeviceIdType.MESH
HIGHEST = lax.Precision.HIGHEST
LAST_WITH_LAST = (((1,), (1,)), ((), ()))
FIRST_WITH_FIRST = (((0,), (0,)), ((), ()))
PLAIN = (((1,), (0,)), ((), ()))
WINDOW = 16
STRIDES = 8


def exact_dot(left, right, dims):
    return lax.dot_general(left, right, dims, precision=HIGHEST, preferred_element_type=jnp.float32)


def pieces(value):
    found = []
    for _ in range(3):
        piece = value.astype(jnp.bfloat16).astype(jnp.float32)
        found.append(piece)
        value = value - piece
    return found


def line_scan(a, lane, upward):
    rows = a.shape[1]
    one, zero = jnp.ones_like(a), jnp.zeros_like(a)

    def behind(v, amount):
        return pltpu.roll(v, amount if upward else rows - amount, 1)

    def inside(amount):
        return lane >= amount if upward else lane < rows - amount

    window = min(WINDOW, rows)
    m = [one, zero, zero, one]
    for i in range(window - 1, -1, -1):
        step = behind(a, i) if i else a
        keep = inside(i)
        for x, y in ((0, 2), (1, 3)):
            total = m[x] + m[y]
            grown = m[x] + step * total
            m[x] = jnp.where(keep, grown, m[x]) if i else grown
            m[y] = jnp.where(keep, total, m[y]) if i else total
    unit = (1.0, 0.0, 0.0, 1.0)
    while window < rows:
        count = min(STRIDES, rows // window)
        terms = [m]
        for i in range(1, count):
            keep = inside(i * window)
            terms.append([jnp.where(keep, behind(v, i * window), u) for v, u in zip(m, unit)])
        while len(terms) > 1:
            joined = []
            for p, q in zip(terms[0::2], terms[1::2]):
                joined.append(
                    [
                        p[0] * q[0] + p[1] * q[2],
                        p[0] * q[1] + p[1] * q[3],
                        p[2] * q[0] + p[3] * q[2],
                        p[2] * q[1] + p[3] * q[3],
                    ]
                )
            terms = joined + terms[2 * len(joined) :]
        m = terms[0]
        window *= count
    return m


def line_factors(a, up, down, before, after, blocks):
    padded, rows = a.shape
    one = jnp.ones_like(a)

    def carried(m, edge, order):
        m = [jnp.broadcast_to(v[:, edge : edge + 1], (padded, rows)) for v in m]
        x, y = one[:1], jnp.zeros_like(one[:1])
        xs, ys, shrink = {}, {}, {}
        for c in order:
            xs[c], ys[c] = x, y
            nx = m[0][c : c + 1] * x + m[1][c : c + 1] * y
            ny = m[2][c : c + 1] * x + m[3][c : c + 1] * y
            ratio = 1.0 / (nx + ny)
            shrink[c] = ratio
            x, y = nx * ratio, ny * ratio
        spare = [one[:1]] * (padded - blocks)
        return [jnp.concatenate([t[c] for c in range(blocks)] + spare, axis=0) for t in (xs, ys, shrink)]

    x_in, y_in, shrink_up = carried(up, rows - 1, range(blocks))
    xb_in, yb_in, shrink_down = carried(down, 0, range(blocks - 1, -1, -1))
    x = up[0] * x_in + up[1] * y_in
    y = up[2] * x_in + up[3] * y_in
    yb = down[2] * xb_in + down[3] * yb_in
    end = lambda v: jnp.broadcast_to(v[:, rows - 1 :], (padded, rows))
    scale = 1.0 / (end(x) + end(y) * xb_in)
    return (
        a * y,
        a * yb,
        y * scale,
        yb * scale,
        shrink_up,
        shrink_down,
        x_in,
        y_in,
        xb_in,
        yb_in,
        -before * y_in,
        after * yb_in,
    )


def kernel(lons, lats, *refs):
    ins, outs, refs = refs[:14], refs[14:17], refs[17:]
    (
        fields,
        land,
        pair,
        wgt,
        slon,
        slat,
        amp,
        factors,
        starts,
        send_lat,
        send_side,
        send_next,
        recv_lat,
        recv_side,
        recv_next,
        recv_sem,
        rim,
        rim_land,
    ) = refs
    a_id = lax.axis_index("lon")
    b_id = lax.axis_index("lat")
    sides = (lax.rem(a_id + lons - 1, lons), lax.rem(a_id + 1, lons))
    znow, depth, hnow, mnow, hold, zold, mold = (fields.at[k] for k in range(7))
    met, cor, samp = pair.at[0], pair.at[1], amp.at[0]
    columns, rows = land.shape
    turns = columns % 128 == 0 and rows % 128 == 0
    padded = wgt.shape[0]

    def early(load_sem, send_sem):
        barrier = pltpu.get_barrier_semaphore()

        def load(group, number, to, at=None):
            source = ins[number] if at is None else ins[number].at[at]
            pltpu.make_async_copy(source, to, load_sem.at[group]).start()

        def loaded(group, ref):
            pltpu.make_async_copy(ref, ref, load_sem.at[group]).wait()

        for k, at in enumerate((0, columns - 1)):
            row = pl.ds(at, 1)
            load(0, 3, rim.at[k, pl.ds(0, 1)], row)
            load(0, 6, rim.at[k, pl.ds(1, 1)], row)
            load(0, 7, rim_land.at[k], row)
            load(0, 1, rim.at[k, pl.ds(2, 1)], row)
        load(1, 8, met)
        load(1, 9, cor)
        load(2, 10, wgt.at[pl.ds(0, lats)])
        load(4, 11, slon)
        load(4, 12, slat)
        load(4, 13, samp)
        for number, slot in ((3, znow), (6, depth), (7, land), (5, mnow), (0, hold), (1, hnow), (2, zold), (4, mold)):
            load(3, number, slot)
        for k in range(1, lats):
            other = lax.rem(b_id + k, lats)
            for column in (*sides, a_id):
                pl.semaphore_signal(barrier, inc=1, device_id=(column, other), device_id_type=MESH)
        for side in sides:
            pl.semaphore_signal(barrier, inc=1, device_id=(side, b_id), device_id_type=MESH)

        loaded(0, rim)
        loaded(1, pair)
        scaled_metric = COURANT * met[...]
        for side, sign in enumerate((-1.0, 1.0)):
            flux = rim[side, 1:2] * rim_land[side].astype(jnp.float32) * rim[side, 0:1]
            flux = sign * scaled_metric * flux
            send_side[side] = flux
            send_next[side] = jnp.concatenate([flux, rim[side, 2:3]], axis=0)

        def remote(src, dst, kind, column, row):
            return pltpu.make_async_remote_copy(
                src_ref=src,
                dst_ref=dst,
                send_sem=send_sem.at[kind],
                recv_sem=recv_sem.at[kind],
                device_id=(column, row),
                device_id_type=MESH,
            )

        def greet_and_send_edges():
            pl.semaphore_wait(barrier, 3 * lats - 1)
            for k in range(1, lats):
                for side in (1, 0):
                    remote(
                        send_side.at[side],
                        recv_side.at[side, lats - k - 1],
                        0,
                        sides[side],
                        lax.rem(b_id + k, lats),
                    ).start()
            for side in (0, 1):
                remote(send_next.at[side], recv_next.at[side], 1, sides[side], b_id).start()

        far = jnp.logical_and(b_id == lats - 1, a_id > 1)
        pl.when(far)(greet_and_send_edges)

        loaded(2, wgt.at[pl.ds(0, lats)])
        loaded(4, amp)
        sources = slon.shape[1]
        east_cell = lax.broadcasted_iota(jnp.int32, (columns, sources), 0) + a_id * columns
        north_cell = lax.broadcasted_iota(jnp.int32, (rows, sources), 0) + b_id * rows
        hit_east = east_cell == slon[...]
        hit_north = jnp.where(north_cell == slat[...], 1.0, 0.0).astype(jnp.bfloat16)
        added = [
            lax.dot_general(
                jnp.where(hit_east, piece, 0.0).astype(jnp.bfloat16),
                hit_north,
                LAST_WITH_LAST,
                preferred_element_type=jnp.float32,
            )
            for piece in pieces(samp[...])
        ]
        added = added[0] + added[1] + added[2]
        weight = wgt[...]
        if padded > lats:
            row_id = lax.broadcasted_iota(jnp.int32, (padded, rows), 0)
            weight = jnp.where(row_id < lats, weight, 1.0)
        a = 1.0 / weight
        lane_of = lax.broadcasted_iota(jnp.int32, (padded, rows), 1)
        first_lane, last_lane = lane_of == 0, lane_of == rows - 1
        before = COURANT * pltpu.roll(jnp.broadcast_to(a[:, rows - 1 :], (padded, rows)), 1, 0)
        after = COURANT * pltpu.roll(jnp.broadcast_to(a[:, :1], (padded, rows)), padded - 1, 0)
        up = line_scan(a, lane_of, True)
        down = line_scan(a, lane_of, False)
        zeros = jnp.zeros_like(a)
        at_last = lambda v: jnp.where(last_lane, v, zeros)
        at_first = lambda v: jnp.where(first_lane, v, zeros)
        for k, value in enumerate(
            (
                a * up[2],
                a * up[3],
                a * down[2],
                a * down[3],
                at_last((up[0] + up[2]) * after),
                at_last((up[1] + up[3]) * after) - at_first(before),
                -at_first((down[0] + down[2]) * before),
                at_last(after) - at_first((down[1] + down[3]) * before),
            )
        ):
            starts[k] = value

        loaded(3, fields)
        wet = land[...].astype(jnp.float32)
        wet_depth = depth[...] * wet
        flux_east = wet_depth * znow[...]
        flux_north = wet_depth * mnow[...]
        metric = met[...]
        line = lax.broadcasted_iota(jnp.int32, (columns, rows), 0)
        lane = lax.broadcasted_iota(jnp.int32, (columns, rows), 1)

        def inner_diff(v, axis, position, size):
            ahead = jnp.where(position == size - 1, 0.0, pltpu.roll(v, size - 1, axis))
            behind = jnp.where(position == 0, 0.0, pltpu.roll(v, 1, axis))
            return ahead - behind

        rhs = added + hold[...] - COURANT * (
            metric * inner_diff(flux_east, 0, line, columns) + inner_diff(flux_north, 1, lane, rows)
        )
        height = hnow[...]
        row_lane = lax.broadcasted_iota(jnp.int32, (1, rows), 1)
        first_row = jnp.where(row_lane == 0, 1.0, 0.0)
        last_row = jnp.where(row_lane == rows - 1, 1.0, 0.0)
        zero_row = jnp.zeros((1, rows), jnp.float32)
        outer = exact_dot(
            jnp.concatenate([zero_row, zero_row, last_row, zero_row] + [zero_row] * 2 + [first_row, zero_row], axis=0),
            height,
            LAST_WITH_LAST,
        )
        def start(k):
            return starts[k, pl.ds(b_id, 1), :]

        def laid(k):
            return jnp.concatenate(
                [start(k), start(k + 1), zero_row, zero_row, start(k + 2), start(k + 3), zero_row, zero_row], axis=0
            )

        moments = outer + exact_dot(
            jnp.concatenate([laid(0), laid(4)], axis=1),
            jnp.concatenate([rhs, flux_north], axis=1),
            LAST_WITH_LAST,
        )
        send_lat[0] = moments[0:4]
        send_lat[1] = moments[4:8]
        pl.when(jnp.logical_not(far))(greet_and_send_edges)
        for k in range(1, lats):
            remote(
                send_lat.at[jnp.where(b_id + k < lats, 0, 1)],
                recv_lat.at[lats - k - 1],
                2,
                a_id,
                lax.rem(b_id + k, lats),
            ).start()

        ends = exact_dot(
            jnp.concatenate([first_row, last_row] + [zero_row] * 6, axis=0), flux_north, LAST_WITH_LAST
        )

        for k, value in enumerate(line_factors(a, up, down, before, after, lats)):
            factors[k] = value

        def own(k, block):
            return factors[k, pl.ds(block, 1), :]

        ay, ayb, y_s, yb_s = [own(k, b_id) for k in range(4)]
        columns_of = jnp.transpose(jnp.concatenate([ay, ayb, yb_s, y_s] + [zero_row] * 4, axis=0))
        source_lat = lax.broadcasted_iota(jnp.int32, (rows, rows), 0)
        target_lat = lax.broadcasted_iota(jnp.int32, (rows, rows), 1)
        below = source_lat <= target_lat
        inverse = jnp.where(below, columns_of[:, 0:1] * yb_s, columns_of[:, 1:2] * y_s)
        outs[0][...] = exact_dot(rhs, inverse, PLAIN)
        turning = cor[...]
        outs[1][...] = wet * (
            zold[...] + turning * mnow[...] - COURANT * metric * inner_diff(height, 0, line, columns)
        )
        outs[2][...] = mold[...] - COURANT * inner_diff(height, 1, lane, rows) - turning * znow[...]

        def across(v):
            return v[:, :columns] if columns <= rows else jnp.broadcast_to(v[:, :1], (1, columns))

        coarse, fine, reach = [None] * lats, [None] * lats, [None] * lats
        product = jnp.ones((1, rows), jnp.float32)
        for d in range(lats - 1, 0, -1):
            block = lax.rem(b_id + d, lats)
            product = product * own(4, block)
            coarse[d], fine[d], reach[d] = own(6, block) * product, own(7, block) * product, own(0, block) * product
        product = jnp.ones((1, rows), jnp.float32)
        for d in range(1, lats):
            block = lax.rem(b_id + d, lats)
            north = b_id + d < lats
            product = product * own(5, block)
            coarse[d] = jnp.where(north, own(8, block) * product, coarse[d])
            fine[d] = jnp.where(north, own(9, block) * product, fine[d])
            reach[d] = jnp.where(north, own(1, block) * product, reach[d])
        own_low = across(own(10, b_id)) * ends[0:1]
        own_high = across(own(11, b_id)) * ends[1:2]
        if turns:
            basis = [jnp.broadcast_to(columns_of[:, k : k + 1], (rows, columns)) for k in (2, 3)]
        else:
            basis = pieces(
                jnp.concatenate(
                    [
                        jnp.concatenate([yb_s, y_s] + [zero_row] * 6, axis=0),
                        jnp.concatenate([zero_row, zero_row, COURANT * first_row, -COURANT * last_row] + [zero_row] * 4, axis=0),
                    ],
                    axis=1,
                )
            )
            basis = jnp.concatenate([basis[k] for k in (0, 1, 2, 0, 1, 0)], axis=0).astype(jnp.bfloat16)
        full = jnp.ones((rows, rows), jnp.float32)
        lower = jnp.where(below, 1.0, 0.0)
        running = jnp.concatenate(
            [jnp.concatenate([lower, full], axis=0), jnp.concatenate([1.0 - lower, full], axis=0)], axis=1
        ).astype(jnp.bfloat16)

        for kind, ref in enumerate((recv_side, recv_next, recv_lat)):
            pltpu.make_async_copy(ref, ref, send_sem.at[kind]).wait()
        return coarse[1:], fine[1:], reach[1:], own_low, own_high, basis, running, ay, ayb, y_s, yb_s

    coarse, fine, reach, own_low, own_high, basis, running, ay, ayb, y_s, yb_s = pl.run_scoped(
        early, pltpu.SemaphoreType.DMA((5,)), pltpu.SemaphoreType.DMA((3,))
    )
    coarse, fine, reach = [None, *coarse], [None, *fine], [None, *reach]

    def across(v):
        return v[:, :columns] if columns <= rows else jnp.broadcast_to(v[:, :1], (1, columns))

    zero_row = jnp.zeros((1, rows), jnp.float32)
    wet, metric = land[...].astype(jnp.float32), met[...]
    arrivals = ((2, recv_lat), (1, recv_next), (0, recv_side))
    for kind, ref in arrivals:
        pltpu.make_async_copy(ref, ref, recv_sem.at[kind]).wait()

    low, high = own_low, own_high
    for d in range(1, lats):
        arrived = recv_lat[d - 1, 0:1] * across(coarse[d]) + recv_lat[d - 1, 1:2] * across(fine[d])
        north = b_id + d < lats
        high = high + jnp.where(north, arrived, 0.0)
        low = low + jnp.where(north, 0.0, arrived)
    south_height = jnp.where(b_id > 0, recv_lat[lats - 2, 2:3], 0.0)
    north_height = jnp.where(b_id < lats - 1, recv_lat[0, 2:3], 0.0)
    if turns:
        lat_at = lax.broadcasted_iota(jnp.int32, (rows, columns), 0)
        outside = jnp.where(
            lat_at == 0, COURANT * south_height, jnp.where(lat_at == rows - 1, -COURANT * north_height, 0.0)
        )
        height_term = jnp.transpose(basis[0] * low + basis[1] * high)
        velocity_term = jnp.transpose(outside)
    else:
        carried = pieces(
            jnp.concatenate([low, high, south_height, north_height, jnp.zeros((4, columns), jnp.float32)], axis=0)
        )
        carried = jnp.concatenate([carried[k] for k in (0, 0, 0, 1, 1, 2)], axis=0).astype(jnp.bfloat16)
        corrections = lax.dot_general(carried, basis, FIRST_WITH_FIRST, preferred_element_type=jnp.float32)
        height_term, velocity_term = corrections[:, :rows], corrections[:, rows:]

    lows, highs = [], []
    for side in (1, 0):
        flux = recv_next[side, 0:1]
        low, high = zero_row, zero_row
        for d in range(1, lats):
            arrived = recv_side[side, d - 1] * reach[d]
            north = b_id + d < lats
            high = high + jnp.where(north, arrived, 0.0)
            low = low + jnp.where(north, 0.0, arrived)
        lows.append(jnp.concatenate([flux * ay, low], axis=1))
        highs.append(jnp.concatenate([flux * ayb, high], axis=1))
    spare = jnp.zeros((4, 2 * rows), jnp.float32)
    edges = jnp.concatenate(pieces(jnp.concatenate(lows + highs + [spare], axis=0)), axis=0)
    edges = jnp.concatenate([edges, jnp.zeros((8, 2 * rows), jnp.float32)], axis=0).astype(jnp.bfloat16)
    edges = lax.dot_general(edges, running, PLAIN, preferred_element_type=jnp.float32)
    edges = edges[0:8] + edges[8:16] + edges[16:24]

    solved = outs[0][...] + height_term
    outs[0][...] = wet * solved
    outs[2][...] = wet * (outs[2][...] + velocity_term)
    for k, (at, side, sign) in enumerate(((0, 1, COURANT), (columns - 1, 0, -COURANT))):
        edge = pl.ds(at, 1)
        outs[0][edge, :] = wet[at : at + 1] * (
            solved[at : at + 1] + edges[k : k + 1, :rows] * yb_s + edges[2 + k : 3 + k, rows:] * y_s
        )
        outs[1][edge, :] = outs[1][edge, :] + wet[at : at + 1] * (sign * metric * recv_next[side, 1:2])


def store_kernel(*refs):
    stores = [
        pltpu.make_async_copy(refs[k], refs[3 + k], refs[6].at[k]) for k in range(3)
    ]
    for store in stores:
        store.start()
    for store in stores:
        store.wait()


def per_device(lons, lats, *args):
    args = list(args)
    columns, rows = args[0].shape
    sources = args[11].shape[0]
    padded = -(-lats // 8) * 8
    args[8] = args[8].reshape(1, rows)
    args[9] = args[9].reshape(1, rows)
    args[10] = args[10].reshape(lats, rows)
    for k in (11, 12, 13):
        args[k] = args[k].reshape(1, sources)
    out = pltpu.VMEM((columns, rows), jnp.float32)
    others = lats - 1
    results = pl.pallas_call(
        functools.partial(kernel, lons, lats),
        out_shape=(out, out, out),
        in_specs=[pl.BlockSpec(memory_space=pl.ANY)] * 14,
        out_specs=(pl.BlockSpec(memory_space=pltpu.VMEM),) * 3,
        scratch_shapes=[
            pltpu.VMEM((8, columns, rows), jnp.float32),
            pltpu.VMEM((columns, rows), jnp.int32),
            pltpu.VMEM((2, 1, rows), jnp.float32),
            pltpu.VMEM((padded, rows), jnp.float32),
            pltpu.VMEM((1, sources), jnp.int32),
            pltpu.VMEM((1, sources), jnp.int32),
            pltpu.VMEM((3, 1, sources), jnp.float32),
            pltpu.VMEM((12, padded, rows), jnp.float32),
            pltpu.VMEM((8, padded, rows), jnp.float32),
            pltpu.VMEM((2, 4, columns), jnp.float32),
            pltpu.VMEM((2, 1, rows), jnp.float32),
            pltpu.VMEM((2, 2, rows), jnp.float32),
            pltpu.VMEM((others, 4, columns), jnp.float32),
            pltpu.VMEM((2, others, 1, rows), jnp.float32),
            pltpu.VMEM((2, 2, rows), jnp.float32),
            pltpu.SemaphoreType.DMA((3,)),
            pltpu.VMEM((2, 4, rows), jnp.float32),
            pltpu.VMEM((2, 1, rows), jnp.int32),
        ],
        compiler_params=pltpu.CompilerParams(collective_id=0, has_side_effects=True),
    )(*args)
    return pl.pallas_call(
        store_kernel,
        out_shape=(jax.ShapeDtypeStruct((columns, rows), jnp.float32),) * 3,
        in_specs=[pl.BlockSpec(memory_space=pltpu.VMEM)] * 3,
        out_specs=(pl.BlockSpec(memory_space=pl.ANY),) * 3,
        scratch_shapes=[pltpu.SemaphoreType.DMA((3,))],
    )(*[pltpu.with_memory_space_constraint(r, pltpu.VMEM) for r in results])


def solution(mesh):
    field = P("lon", "lat")
    placed = (field,) * 8 + (P("lat"),) * 2 + (P(),) * 4
    return jax.shard_map(
        functools.partial(per_device, mesh.shape["lon"], mesh.shape["lat"]),
        mesh=mesh,
        in_specs=placed,
        out_specs=(field,) * 3,
        check_vma=False,
    )
```

```python
import functools

import jax
import jax.numpy as jnp
from jax import lax
from jax.experimental import pallas as pl
from jax.experimental.pallas import tpu as pltpu
from jax.sharding import PartitionSpec as P

COURANT = 0.25
MESH = pl.DeviceIdType.MESH
HIGHEST = lax.Precision.HIGHEST
LAST_WITH_LAST = (((1,), (1,)), ((), ()))
FIRST_WITH_FIRST = (((0,), (0,)), ((), ()))
PLAIN = (((1,), (0,)), ((), ()))
WINDOW = 16
STRIDES = 8


def exact_dot(left, right, dims):
    return lax.dot_general(left, right, dims, precision=HIGHEST, preferred_element_type=jnp.float32)


def pieces(value):
    found = []
    for _ in range(3):
        piece = value.astype(jnp.bfloat16).astype(jnp.float32)
        found.append(piece)
        value = value - piece
    return found


def line_scan(a, lane, upward):
    rows = a.shape[1]
    one, zero = jnp.ones_like(a), jnp.zeros_like(a)

    def behind(v, amount):
        return pltpu.roll(v, amount if upward else rows - amount, 1)

    def inside(amount):
        return lane >= amount if upward else lane < rows - amount

    window = min(WINDOW, rows)
    m = [one, zero, zero, one]
    for i in range(window - 1, -1, -1):
        step = behind(a, i) if i else a
        keep = inside(i)
        for x, y in ((0, 2), (1, 3)):
            total = m[x] + m[y]
            grown = m[x] + step * total
            m[x] = jnp.where(keep, grown, m[x]) if i else grown
            m[y] = jnp.where(keep, total, m[y]) if i else total
    unit = (1.0, 0.0, 0.0, 1.0)
    while window < rows:
        count = min(STRIDES, rows // window)
        terms = [m]
        for i in range(1, count):
            keep = inside(i * window)
            terms.append([jnp.where(keep, behind(v, i * window), u) for v, u in zip(m, unit)])
        while len(terms) > 1:
            joined = []
            for p, q in zip(terms[0::2], terms[1::2]):
                joined.append(
                    [
                        p[0] * q[0] + p[1] * q[2],
                        p[0] * q[1] + p[1] * q[3],
                        p[2] * q[0] + p[3] * q[2],
                        p[2] * q[1] + p[3] * q[3],
                    ]
                )
            terms = joined + terms[2 * len(joined) :]
        m = terms[0]
        window *= count
    return m


def line_factors(a, up, down, before, after, blocks):
    padded, rows = a.shape
    one = jnp.ones_like(a)

    def carried(m, edge, order):
        m = [jnp.broadcast_to(v[:, edge : edge + 1], (padded, rows)) for v in m]
        x, y = one[:1], jnp.zeros_like(one[:1])
        xs, ys, shrink = {}, {}, {}
        for c in order:
            xs[c], ys[c] = x, y
            nx = m[0][c : c + 1] * x + m[1][c : c + 1] * y
            ny = m[2][c : c + 1] * x + m[3][c : c + 1] * y
            ratio = 1.0 / (nx + ny)
            shrink[c] = ratio
            x, y = nx * ratio, ny * ratio
        spare = [one[:1]] * (padded - blocks)
        return [jnp.concatenate([t[c] for c in range(blocks)] + spare, axis=0) for t in (xs, ys, shrink)]

    x_in, y_in, shrink_up = carried(up, rows - 1, range(blocks))
    xb_in, yb_in, shrink_down = carried(down, 0, range(blocks - 1, -1, -1))
    x = up[0] * x_in + up[1] * y_in
    y = up[2] * x_in + up[3] * y_in
    yb = down[2] * xb_in + down[3] * yb_in
    end = lambda v: jnp.broadcast_to(v[:, rows - 1 :], (padded, rows))
    scale = 1.0 / (end(x) + end(y) * xb_in)
    return (
        a * y,
        a * yb,
        y * scale,
        yb * scale,
        shrink_up,
        shrink_down,
        x_in,
        y_in,
        xb_in,
        yb_in,
        -before * y_in,
        after * yb_in,
    )


def kernel(lons, lats, *refs):
    ins, outs, refs = refs[:14], refs[14:17], refs[17:]
    (
        fields,
        land,
        pair,
        wgt,
        slon,
        slat,
        amp,
        factors,
        starts,
        send_lat,
        send_side,
        send_next,
        recv_lat,
        recv_side,
        recv_next,
        recv_sem,
        rim,
        rim_land,
    ) = refs
    a_id = lax.axis_index("lon")
    b_id = lax.axis_index("lat")
    sides = (lax.rem(a_id + lons - 1, lons), lax.rem(a_id + 1, lons))
    znow, depth, hnow, mnow, hold, zold, mold = (fields.at[k] for k in range(7))
    met, cor, samp = pair.at[0], pair.at[1], amp.at[0]
    columns, rows = land.shape
    trims = lats >= 4 and lats % 2 == 0
    lat_bytes = recv_lat.at[pl.ds(0, lats // 2)] if trims else recv_lat

    def part(k):
        return pl.ds(0, (3 if k in (1, lats - 1) else 2) if trims else 4)

    turns = columns % 128 == 0 and rows % 128 == 0
    padded = wgt.shape[0]

    def early(load_sem, send_sem):
        barrier = pltpu.get_barrier_semaphore()

        def load(group, number, to, at=None):
            source = ins[number] if at is None else ins[number].at[at]
            pltpu.make_async_copy(source, to, load_sem.at[group]).start()

        def loaded(group, ref):
            pltpu.make_async_copy(ref, ref, load_sem.at[group]).wait()

        for k, at in enumerate((0, columns - 1)):
            row = pl.ds(at, 1)
            load(0, 3, rim.at[k, pl.ds(0, 1)], row)
            load(0, 6, rim.at[k, pl.ds(1, 1)], row)
            load(0, 7, rim_land.at[k], row)
            load(0, 1, rim.at[k, pl.ds(2, 1)], row)
        load(1, 8, met)
        load(1, 9, cor)
        load(2, 10, wgt.at[pl.ds(0, lats)])
        load(4, 11, slon)
        load(4, 12, slat)
        load(4, 13, samp)
        for number, slot in ((3, znow), (6, depth), (7, land), (5, mnow), (0, hold), (1, hnow), (2, zold), (4, mold)):
            load(3, number, slot)
        for k in range(1, lats):
            other = lax.rem(b_id + k, lats)
            for column in (*sides, a_id):
                pl.semaphore_signal(barrier, inc=1, device_id=(column, other), device_id_type=MESH)
        for side in sides:
            pl.semaphore_signal(barrier, inc=1, device_id=(side, b_id), device_id_type=MESH)

        loaded(0, rim)
        loaded(1, pair)
        scaled_metric = COURANT * met[...]
        for side, sign in enumerate((-1.0, 1.0)):
            flux = rim[side, 1:2] * rim_land[side].astype(jnp.float32) * rim[side, 0:1]
            flux = sign * scaled_metric * flux
            send_side[side] = flux
            send_next[side] = jnp.concatenate([flux, rim[side, 2:3]], axis=0)

        def remote(src, dst, kind, column, row):
            return pltpu.make_async_remote_copy(
                src_ref=src,
                dst_ref=dst,
                send_sem=send_sem.at[kind],
                recv_sem=recv_sem.at[kind],
                device_id=(column, row),
                device_id_type=MESH,
            )

        def greet_and_send_edges():
            pl.semaphore_wait(barrier, 3 * lats - 1)
            for k in range(1, lats):
                for side in (1, 0):
                    remote(
                        send_side.at[side],
                        recv_side.at[side, lats - k - 1],
                        0,
                        sides[side],
                        lax.rem(b_id + k, lats),
                    ).start()
            for side in (0, 1):
                remote(send_next.at[side], recv_next.at[side], 1, sides[side], b_id).start()

        far = jnp.logical_and(b_id == lats - 1, a_id > 1)
        pl.when(far)(greet_and_send_edges)

        loaded(2, wgt.at[pl.ds(0, lats)])
        loaded(4, amp)
        sources = slon.shape[1]
        east_cell = lax.broadcasted_iota(jnp.int32, (columns, sources), 0) + a_id * columns
        north_cell = lax.broadcasted_iota(jnp.int32, (rows, sources), 0) + b_id * rows
        hit_east = east_cell == slon[...]
        hit_north = jnp.where(north_cell == slat[...], 1.0, 0.0).astype(jnp.bfloat16)
        added = [
            lax.dot_general(
                jnp.where(hit_east, piece, 0.0).astype(jnp.bfloat16),
                hit_north,
                LAST_WITH_LAST,
                preferred_element_type=jnp.float32,
            )
            for piece in pieces(samp[...])
        ]
        added = added[0] + added[1] + added[2]
        weight = wgt[...]
        if padded > lats:
            row_id = lax.broadcasted_iota(jnp.int32, (padded, rows), 0)
            weight = jnp.where(row_id < lats, weight, 1.0)
        a = 1.0 / weight
        lane_of = lax.broadcasted_iota(jnp.int32, (padded, rows), 1)
        first_lane, last_lane = lane_of == 0, lane_of == rows - 1
        before = COURANT * pltpu.roll(jnp.broadcast_to(a[:, rows - 1 :], (padded, rows)), 1, 0)
        after = COURANT * pltpu.roll(jnp.broadcast_to(a[:, :1], (padded, rows)), padded - 1, 0)
        up = line_scan(a, lane_of, True)
        down = line_scan(a, lane_of, False)
        zeros = jnp.zeros_like(a)
        at_last = lambda v: jnp.where(last_lane, v, zeros)
        at_first = lambda v: jnp.where(first_lane, v, zeros)
        for k, value in enumerate(
            (
                a * up[2],
                a * up[3],
                a * down[2],
                a * down[3],
                at_last((up[0] + up[2]) * after),
                at_last((up[1] + up[3]) * after) - at_first(before),
                -at_first((down[0] + down[2]) * before),
                at_last(after) - at_first((down[1] + down[3]) * before),
            )
        ):
            starts[k] = value

        loaded(3, fields)
        wet = land[...].astype(jnp.float32)
        wet_depth = depth[...] * wet
        flux_east = wet_depth * znow[...]
        flux_north = wet_depth * mnow[...]
        metric = met[...]
        line = lax.broadcasted_iota(jnp.int32, (columns, rows), 0)
        lane = lax.broadcasted_iota(jnp.int32, (columns, rows), 1)

        def inner_diff(v, axis, position, size):
            ahead = jnp.where(position == size - 1, 0.0, pltpu.roll(v, size - 1, axis))
            behind = jnp.where(position == 0, 0.0, pltpu.roll(v, 1, axis))
            return ahead - behind

        rhs = added + hold[...] - COURANT * (
            metric * inner_diff(flux_east, 0, line, columns) + inner_diff(flux_north, 1, lane, rows)
        )
        height = hnow[...]
        row_lane = lax.broadcasted_iota(jnp.int32, (1, rows), 1)
        first_row = jnp.where(row_lane == 0, 1.0, 0.0)
        last_row = jnp.where(row_lane == rows - 1, 1.0, 0.0)
        zero_row = jnp.zeros((1, rows), jnp.float32)
        outer = exact_dot(
            jnp.concatenate([zero_row, zero_row, last_row, zero_row] + [zero_row] * 2 + [first_row, zero_row], axis=0),
            height,
            LAST_WITH_LAST,
        )
        def start(k):
            return starts[k, pl.ds(b_id, 1), :]

        def laid(k):
            return jnp.concatenate(
                [start(k), start(k + 1), zero_row, zero_row, start(k + 2), start(k + 3), zero_row, zero_row], axis=0
            )

        moments = outer + exact_dot(
            jnp.concatenate([laid(0), laid(4)], axis=1),
            jnp.concatenate([rhs, flux_north], axis=1),
            LAST_WITH_LAST,
        )
        send_lat[0] = moments[0:4]
        send_lat[1] = moments[4:8]
        pl.when(jnp.logical_not(far))(greet_and_send_edges)
        for k in range(1, lats):
            remote(
                send_lat.at[jnp.where(b_id + k < lats, 0, 1), part(k)],
                recv_lat.at[lats - k - 1, part(k)],
                2,
                a_id,
                lax.rem(b_id + k, lats),
            ).start()

        ends = exact_dot(
            jnp.concatenate([first_row, last_row] + [zero_row] * 6, axis=0), flux_north, LAST_WITH_LAST
        )

        for k, value in enumerate(line_factors(a, up, down, before, after, lats)):
            factors[k] = value

        def own(k, block):
            return factors[k, pl.ds(block, 1), :]

        ay, ayb, y_s, yb_s = [own(k, b_id) for k in range(4)]
        columns_of = jnp.transpose(jnp.concatenate([ay, ayb, yb_s, y_s] + [zero_row] * 4, axis=0))
        source_lat = lax.broadcasted_iota(jnp.int32, (rows, rows), 0)
        target_lat = lax.broadcasted_iota(jnp.int32, (rows, rows), 1)
        below = source_lat <= target_lat
        inverse = jnp.where(below, columns_of[:, 0:1] * yb_s, columns_of[:, 1:2] * y_s)
        outs[0][...] = exact_dot(rhs, inverse, PLAIN)
        turning = cor[...]
        outs[1][...] = wet * (
            zold[...] + turning * mnow[...] - COURANT * metric * inner_diff(height, 0, line, columns)
        )
        outs[2][...] = mold[...] - COURANT * inner_diff(height, 1, lane, rows) - turning * znow[...]

        def across(v):
            return v[:, :columns] if columns <= rows else jnp.broadcast_to(v[:, :1], (1, columns))

        coarse, fine, reach = [None] * lats, [None] * lats, [None] * lats
        product = jnp.ones((1, rows), jnp.float32)
        for d in range(lats - 1, 0, -1):
            block = lax.rem(b_id + d, lats)
            product = product * own(4, block)
            coarse[d], fine[d], reach[d] = own(6, block) * product, own(7, block) * product, own(0, block) * product
        product = jnp.ones((1, rows), jnp.float32)
        for d in range(1, lats):
            block = lax.rem(b_id + d, lats)
            north = b_id + d < lats
            product = product * own(5, block)
            coarse[d] = jnp.where(north, own(8, block) * product, coarse[d])
            fine[d] = jnp.where(north, own(9, block) * product, fine[d])
            reach[d] = jnp.where(north, own(1, block) * product, reach[d])
        own_low = across(own(10, b_id)) * ends[0:1]
        own_high = across(own(11, b_id)) * ends[1:2]
        if turns:
            basis = [jnp.broadcast_to(columns_of[:, k : k + 1], (rows, columns)) for k in (2, 3)]
        else:
            basis = pieces(
                jnp.concatenate(
                    [
                        jnp.concatenate([yb_s, y_s] + [zero_row] * 6, axis=0),
                        jnp.concatenate([zero_row, zero_row, COURANT * first_row, -COURANT * last_row] + [zero_row] * 4, axis=0),
                    ],
                    axis=1,
                )
            )
            basis = jnp.concatenate([basis[k] for k in (0, 1, 2, 0, 1, 0)], axis=0).astype(jnp.bfloat16)
        full = jnp.ones((rows, rows), jnp.float32)
        lower = jnp.where(below, 1.0, 0.0)
        running = jnp.concatenate(
            [jnp.concatenate([lower, full], axis=0), jnp.concatenate([1.0 - lower, full], axis=0)], axis=1
        ).astype(jnp.bfloat16)

        for kind, ref in enumerate((recv_side, recv_next, lat_bytes)):
            pltpu.make_async_copy(ref, ref, send_sem.at[kind]).wait()
        return coarse[1:], fine[1:], reach[1:], own_low, own_high, basis, running, ay, ayb, y_s, yb_s

    coarse, fine, reach, own_low, own_high, basis, running, ay, ayb, y_s, yb_s = pl.run_scoped(
        early, pltpu.SemaphoreType.DMA((5,)), pltpu.SemaphoreType.DMA((3,))
    )
    coarse, fine, reach = [None, *coarse], [None, *fine], [None, *reach]

    def across(v):
        return v[:, :columns] if columns <= rows else jnp.broadcast_to(v[:, :1], (1, columns))

    zero_row = jnp.zeros((1, rows), jnp.float32)
    wet, metric = land[...].astype(jnp.float32), met[...]
    arrivals = ((1, recv_next), (0, recv_side), (2, lat_bytes))
    for kind, ref in arrivals:
        pltpu.make_async_copy(ref, ref, recv_sem.at[kind]).wait()

    low, high = own_low, own_high
    for d in range(1, lats):
        arrived = recv_lat[d - 1, 0:1] * across(coarse[d]) + recv_lat[d - 1, 1:2] * across(fine[d])
        north = b_id + d < lats
        high = high + jnp.where(north, arrived, 0.0)
        low = low + jnp.where(north, 0.0, arrived)
    south_height = jnp.where(b_id > 0, recv_lat[lats - 2, 2:3], 0.0)
    north_height = jnp.where(b_id < lats - 1, recv_lat[0, 2:3], 0.0)
    if turns:
        lat_at = lax.broadcasted_iota(jnp.int32, (rows, columns), 0)
        outside = jnp.where(
            lat_at == 0, COURANT * south_height, jnp.where(lat_at == rows - 1, -COURANT * north_height, 0.0)
        )
        height_term = jnp.transpose(basis[0] * low + basis[1] * high)
        velocity_term = jnp.transpose(outside)
    else:
        carried = pieces(
            jnp.concatenate([low, high, south_height, north_height, jnp.zeros((4, columns), jnp.float32)], axis=0)
        )
        carried = jnp.concatenate([carried[k] for k in (0, 0, 0, 1, 1, 2)], axis=0).astype(jnp.bfloat16)
        corrections = lax.dot_general(carried, basis, FIRST_WITH_FIRST, preferred_element_type=jnp.float32)
        height_term, velocity_term = corrections[:, :rows], corrections[:, rows:]

    lows, highs = [], []
    for side in (1, 0):
        flux = recv_next[side, 0:1]
        low, high = zero_row, zero_row
        for d in range(1, lats):
            arrived = recv_side[side, d - 1] * reach[d]
            north = b_id + d < lats
            high = high + jnp.where(north, arrived, 0.0)
            low = low + jnp.where(north, 0.0, arrived)
        lows.append(jnp.concatenate([flux * ay, low], axis=1))
        highs.append(jnp.concatenate([flux * ayb, high], axis=1))
    spare = jnp.zeros((4, 2 * rows), jnp.float32)
    edges = jnp.concatenate(pieces(jnp.concatenate(lows + highs + [spare], axis=0)), axis=0)
    edges = jnp.concatenate([edges, jnp.zeros((8, 2 * rows), jnp.float32)], axis=0).astype(jnp.bfloat16)
    edges = lax.dot_general(edges, running, PLAIN, preferred_element_type=jnp.float32)
    edges = edges[0:8] + edges[8:16] + edges[16:24]

    solved = outs[0][...] + height_term
    outs[0][...] = wet * solved
    outs[2][...] = wet * (outs[2][...] + velocity_term)
    for k, (at, side, sign) in enumerate(((0, 1, COURANT), (columns - 1, 0, -COURANT))):
        edge = pl.ds(at, 1)
        outs[0][edge, :] = wet[at : at + 1] * (
            solved[at : at + 1] + edges[k : k + 1, :rows] * yb_s + edges[2 + k : 3 + k, rows:] * y_s
        )
        outs[1][edge, :] = outs[1][edge, :] + wet[at : at + 1] * (sign * metric * recv_next[side, 1:2])


def store_kernel(*refs):
    def move(sem):
        stores = [pltpu.make_async_copy(refs[k], refs[3 + k], sem.at[k]) for k in range(3)]
        for store in stores:
            store.start()
        for store in stores:
            store.wait()

    pl.run_scoped(move, pltpu.SemaphoreType.DMA((3,)))


def per_device(lons, lats, *args):
    args = list(args)
    columns, rows = args[0].shape
    sources = args[11].shape[0]
    padded = -(-lats // 8) * 8
    args[8] = args[8].reshape(1, rows)
    args[9] = args[9].reshape(1, rows)
    args[10] = args[10].reshape(lats, rows)
    for k in (11, 12, 13):
        args[k] = args[k].reshape(1, sources)
    out = pltpu.VMEM((columns, rows), jnp.float32)
    others = lats - 1
    results = pl.pallas_call(
        functools.partial(kernel, lons, lats),
        out_shape=(out, out, out),
        in_specs=[pl.BlockSpec(memory_space=pl.ANY)] * 14,
        out_specs=(pl.BlockSpec(memory_space=pltpu.VMEM),) * 3,
        scratch_shapes=[
            pltpu.VMEM((8, columns, rows), jnp.float32),
            pltpu.VMEM((columns, rows), jnp.int32),
            pltpu.VMEM((2, 1, rows), jnp.float32),
            pltpu.VMEM((padded, rows), jnp.float32),
            pltpu.VMEM((1, sources), jnp.int32),
            pltpu.VMEM((1, sources), jnp.int32),
            pltpu.VMEM((3, 1, sources), jnp.float32),
            pltpu.VMEM((12, padded, rows), jnp.float32),
            pltpu.VMEM((8, padded, rows), jnp.float32),
            pltpu.VMEM((2, 4, columns), jnp.float32),
            pltpu.VMEM((2, 1, rows), jnp.float32),
            pltpu.VMEM((2, 2, rows), jnp.float32),
            pltpu.VMEM((others, 4, columns), jnp.float32),
            pltpu.VMEM((2, others, 1, rows), jnp.float32),
            pltpu.VMEM((2, 2, rows), jnp.float32),
            pltpu.SemaphoreType.DMA((3,)),
            pltpu.VMEM((2, 4, rows), jnp.float32),
            pltpu.VMEM((2, 1, rows), jnp.int32),
        ],
        compiler_params=pltpu.CompilerParams(collective_id=0, has_side_effects=True),
    )(*args)
    return pl.pallas_call(
        store_kernel,
        out_shape=(jax.ShapeDtypeStruct((columns, rows), jnp.float32),) * 3,
        in_specs=[pl.BlockSpec(memory_space=pltpu.VMEM)] * 3,
        out_specs=(pl.BlockSpec(memory_space=pl.ANY),) * 3,
    )(*[pltpu.with_memory_space_constraint(r, pltpu.VMEM) for r in results])


def solution(mesh):
    field = P("lon", "lat")
    placed = (field,) * 8 + (P("lat"),) * 2 + (P(),) * 4
    return jax.shard_map(
        functools.partial(per_device, mesh.shape["lon"], mesh.shape["lat"]),
        mesh=mesh,
        in_specs=placed,
        out_specs=(field,) * 3,
        check_vma=False,
    )
```

```python
import functools

import jax
import jax.numpy as jnp
from jax import lax
from jax.experimental import pallas as pl
from jax.experimental.pallas import tpu as pltpu
from jax.sharding import PartitionSpec as P

COURANT = 0.25
MESH = pl.DeviceIdType.MESH
HIGHEST = lax.Precision.HIGHEST
LAST_WITH_LAST = (((1,), (1,)), ((), ()))
FIRST_WITH_FIRST = (((0,), (0,)), ((), ()))
PLAIN = (((1,), (0,)), ((), ()))
WINDOW = 16
STRIDES = 8


def exact_dot(left, right, dims):
    return lax.dot_general(left, right, dims, precision=HIGHEST, preferred_element_type=jnp.float32)


def pieces(value):
    found = []
    for _ in range(3):
        piece = value.astype(jnp.bfloat16).astype(jnp.float32)
        found.append(piece)
        value = value - piece
    return found


def line_scan(a, lane, upward):
    rows = a.shape[1]
    one, zero = jnp.ones_like(a), jnp.zeros_like(a)

    def behind(v, amount):
        return pltpu.roll(v, amount if upward else rows - amount, 1)

    def inside(amount):
        return lane >= amount if upward else lane < rows - amount

    window = min(WINDOW, rows)
    m = [one, zero, zero, one]
    for i in range(window - 1, -1, -1):
        step = behind(a, i) if i else a
        keep = inside(i)
        for x, y in ((0, 2), (1, 3)):
            total = m[x] + m[y]
            grown = m[x] + step * total
            m[x] = jnp.where(keep, grown, m[x]) if i else grown
            m[y] = jnp.where(keep, total, m[y]) if i else total
    unit = (1.0, 0.0, 0.0, 1.0)
    while window < rows:
        count = min(STRIDES, rows // window)
        terms = [m]
        for i in range(1, count):
            keep = inside(i * window)
            terms.append([jnp.where(keep, behind(v, i * window), u) for v, u in zip(m, unit)])
        while len(terms) > 1:
            joined = []
            for p, q in zip(terms[0::2], terms[1::2]):
                joined.append(
                    [
                        p[0] * q[0] + p[1] * q[2],
                        p[0] * q[1] + p[1] * q[3],
                        p[2] * q[0] + p[3] * q[2],
                        p[2] * q[1] + p[3] * q[3],
                    ]
                )
            terms = joined + terms[2 * len(joined) :]
        m = terms[0]
        window *= count
    return m


def line_factors(a, up, down, before, after, blocks):
    padded, rows = a.shape
    one = jnp.ones_like(a)

    def carried(m, edge, order):
        m = [jnp.broadcast_to(v[:, edge : edge + 1], (padded, rows)) for v in m]
        x, y = one[:1], jnp.zeros_like(one[:1])
        xs, ys, shrink = {}, {}, {}
        for c in order:
            xs[c], ys[c] = x, y
            nx = m[0][c : c + 1] * x + m[1][c : c + 1] * y
            ny = m[2][c : c + 1] * x + m[3][c : c + 1] * y
            ratio = 1.0 / (nx + ny)
            shrink[c] = ratio
            x, y = nx * ratio, ny * ratio
        spare = [one[:1]] * (padded - blocks)
        return [jnp.concatenate([t[c] for c in range(blocks)] + spare, axis=0) for t in (xs, ys, shrink)]

    x_in, y_in, shrink_up = carried(up, rows - 1, range(blocks))
    xb_in, yb_in, shrink_down = carried(down, 0, range(blocks - 1, -1, -1))
    x = up[0] * x_in + up[1] * y_in
    y = up[2] * x_in + up[3] * y_in
    yb = down[2] * xb_in + down[3] * yb_in
    end = lambda v: jnp.broadcast_to(v[:, rows - 1 :], (padded, rows))
    scale = 1.0 / (end(x) + end(y) * xb_in)
    return (
        a * y,
        a * yb,
        y * scale,
        yb * scale,
        shrink_up,
        shrink_down,
        x_in,
        y_in,
        xb_in,
        yb_in,
        -before * y_in,
        after * yb_in,
    )


def kernel(lons, lats, *refs):
    ins, outs, refs = refs[:14], refs[14:17], refs[17:]
    (
        fields,
        land,
        pair,
        wgt,
        slon,
        slat,
        amp,
        factors,
        starts,
        send_lat,
        send_side,
        send_next,
        recv_lat,
        recv_side,
        recv_next,
        recv_sem,
        rim,
        rim_land,
    ) = refs
    a_id = lax.axis_index("lon")
    b_id = lax.axis_index("lat")
    sides = (lax.rem(a_id + lons - 1, lons), lax.rem(a_id + 1, lons))
    znow, depth, hnow, mnow, hold, zold, mold = (fields.at[k] for k in range(7))
    met, cor, samp = pair.at[0], pair.at[1], amp.at[0]
    columns, rows = land.shape
    trims = lats >= 4 and lats % 2 == 0
    lat_bytes = recv_lat.at[pl.ds(0, lats // 2)] if trims else recv_lat

    def part(k):
        return pl.ds(0, (3 if k in (1, lats - 1) else 2) if trims else 4)

    turns = columns % 128 == 0 and rows % 128 == 0
    padded = wgt.shape[0]

    def early(load_sem, send_sem):
        barrier = pltpu.get_barrier_semaphore()

        def load(group, number, to, at=None):
            source = ins[number] if at is None else ins[number].at[at]
            pltpu.make_async_copy(source, to, load_sem.at[group]).start()

        def loaded(group, ref):
            pltpu.make_async_copy(ref, ref, load_sem.at[group]).wait()

        for k, at in enumerate((0, columns - 1)):
            row = pl.ds(at, 1)
            load(0, 3, rim.at[k, pl.ds(0, 1)], row)
            load(0, 6, rim.at[k, pl.ds(1, 1)], row)
            load(0, 7, rim_land.at[k], row)
            load(0, 1, rim.at[k, pl.ds(2, 1)], row)
        load(1, 8, met)
        load(1, 9, cor)
        load(2, 10, wgt.at[pl.ds(0, lats)])
        load(4, 11, slon)
        load(4, 12, slat)
        load(4, 13, samp)
        south_half = 2 * b_id < lats
        for k in range(lats - 1):
            down, up_row = lats - 1 - k, k
            down = down - (down <= b_id).astype(jnp.int32)
            up_row = up_row + (up_row >= b_id).astype(jnp.int32)
            other = jnp.where(south_half, down, up_row)
            for column in (*sides, a_id):
                pl.semaphore_signal(barrier, inc=1, device_id=(column, other), device_id_type=MESH)
            if k == 0:
                for side in sides:
                    pl.semaphore_signal(barrier, inc=1, device_id=(side, b_id), device_id_type=MESH)
        for number, slot in ((3, znow), (6, depth), (7, land), (5, mnow), (0, hold), (1, hnow), (2, zold), (4, mold)):
            load(3, number, slot)

        loaded(0, rim)
        loaded(1, pair)
        scaled_metric = COURANT * met[...]
        for side, sign in enumerate((-1.0, 1.0)):
            flux = rim[side, 1:2] * rim_land[side].astype(jnp.float32) * rim[side, 0:1]
            flux = sign * scaled_metric * flux
            send_side[side] = flux
            send_next[side] = jnp.concatenate([flux, rim[side, 2:3]], axis=0)

        def remote(src, dst, kind, column, row):
            return pltpu.make_async_remote_copy(
                src_ref=src,
                dst_ref=dst,
                send_sem=send_sem.at[kind],
                recv_sem=recv_sem.at[kind],
                device_id=(column, row),
                device_id_type=MESH,
            )

        def greet_and_send_edges():
            pl.semaphore_wait(barrier, 3 * lats - 1)
            for k in range(1, lats):
                for side in (1, 0):
                    remote(
                        send_side.at[side],
                        recv_side.at[side, lats - k - 1],
                        0,
                        sides[side],
                        lax.rem(b_id + k, lats),
                    ).start()
            for side in (0, 1):
                remote(send_next.at[side], recv_next.at[side], 1, sides[side], b_id).start()

        far = jnp.logical_and(b_id == lats - 1, a_id > 1)
        pl.when(far)(greet_and_send_edges)

        loaded(2, wgt.at[pl.ds(0, lats)])
        loaded(4, amp)
        sources = slon.shape[1]
        east_cell = lax.broadcasted_iota(jnp.int32, (columns, sources), 0) + a_id * columns
        north_cell = lax.broadcasted_iota(jnp.int32, (rows, sources), 0) + b_id * rows
        hit_east = east_cell == slon[...]
        hit_north = jnp.where(north_cell == slat[...], 1.0, 0.0).astype(jnp.bfloat16)
        added = [
            lax.dot_general(
                jnp.where(hit_east, piece, 0.0).astype(jnp.bfloat16),
                hit_north,
                LAST_WITH_LAST,
                preferred_element_type=jnp.float32,
            )
            for piece in pieces(samp[...])
        ]
        added = added[0] + added[1] + added[2]
        weight = wgt[...]
        if padded > lats:
            row_id = lax.broadcasted_iota(jnp.int32, (padded, rows), 0)
            weight = jnp.where(row_id < lats, weight, 1.0)
        a = 1.0 / weight
        lane_of = lax.broadcasted_iota(jnp.int32, (padded, rows), 1)
        first_lane, last_lane = lane_of == 0, lane_of == rows - 1
        before = COURANT * pltpu.roll(jnp.broadcast_to(a[:, rows - 1 :], (padded, rows)), 1, 0)
        after = COURANT * pltpu.roll(jnp.broadcast_to(a[:, :1], (padded, rows)), padded - 1, 0)
        up = line_scan(a, lane_of, True)
        down = line_scan(a, lane_of, False)
        zeros = jnp.zeros_like(a)
        at_last = lambda v: jnp.where(last_lane, v, zeros)
        at_first = lambda v: jnp.where(first_lane, v, zeros)
        for k, value in enumerate(
            (
                a * up[2],
                a * up[3],
                a * down[2],
                a * down[3],
                at_last((up[0] + up[2]) * after),
                at_last((up[1] + up[3]) * after) - at_first(before),
                -at_first((down[0] + down[2]) * before),
                at_last(after) - at_first((down[1] + down[3]) * before),
            )
        ):
            starts[k] = value

        loaded(3, fields)
        wet = land[...].astype(jnp.float32)
        wet_depth = depth[...] * wet
        flux_east = wet_depth * znow[...]
        flux_north = wet_depth * mnow[...]
        metric = met[...]
        line = lax.broadcasted_iota(jnp.int32, (columns, rows), 0)
        lane = lax.broadcasted_iota(jnp.int32, (columns, rows), 1)

        def inner_diff(v, axis, position, size):
            ahead = jnp.where(position == size - 1, 0.0, pltpu.roll(v, size - 1, axis))
            behind = jnp.where(position == 0, 0.0, pltpu.roll(v, 1, axis))
            return ahead - behind

        rhs = added + hold[...] - COURANT * (
            metric * inner_diff(flux_east, 0, line, columns) + inner_diff(flux_north, 1, lane, rows)
        )
        height = hnow[...]
        row_lane = lax.broadcasted_iota(jnp.int32, (1, rows), 1)
        first_row = jnp.where(row_lane == 0, 1.0, 0.0)
        last_row = jnp.where(row_lane == rows - 1, 1.0, 0.0)
        zero_row = jnp.zeros((1, rows), jnp.float32)
        outer = exact_dot(
            jnp.concatenate([zero_row, zero_row, last_row, zero_row] + [zero_row] * 2 + [first_row, zero_row], axis=0),
            height,
            LAST_WITH_LAST,
        )
        def start(k):
            return starts[k, pl.ds(b_id, 1), :]

        def laid(k):
            return jnp.concatenate(
                [start(k), start(k + 1), zero_row, zero_row, start(k + 2), start(k + 3), zero_row, zero_row], axis=0
            )

        moments = outer + exact_dot(
            jnp.concatenate([laid(0), laid(4)], axis=1),
            jnp.concatenate([rhs, flux_north], axis=1),
            LAST_WITH_LAST,
        )
        send_lat[0] = moments[0:4]
        send_lat[1] = moments[4:8]
        pl.when(jnp.logical_not(far))(greet_and_send_edges)
        for k in range(1, lats):
            remote(
                send_lat.at[jnp.where(b_id + k < lats, 0, 1), part(k)],
                recv_lat.at[lats - k - 1, part(k)],
                2,
                a_id,
                lax.rem(b_id + k, lats),
            ).start()

        ends = exact_dot(
            jnp.concatenate([first_row, last_row] + [zero_row] * 6, axis=0), flux_north, LAST_WITH_LAST
        )

        for k, value in enumerate(line_factors(a, up, down, before, after, lats)):
            factors[k] = value

        def own(k, block):
            return factors[k, pl.ds(block, 1), :]

        ay, ayb, y_s, yb_s = [own(k, b_id) for k in range(4)]
        columns_of = jnp.transpose(jnp.concatenate([ay, ayb, yb_s, y_s] + [zero_row] * 4, axis=0))
        source_lat = lax.broadcasted_iota(jnp.int32, (rows, rows), 0)
        target_lat = lax.broadcasted_iota(jnp.int32, (rows, rows), 1)
        below = source_lat <= target_lat
        inverse = jnp.where(below, columns_of[:, 0:1] * yb_s, columns_of[:, 1:2] * y_s)
        outs[0][...] = exact_dot(rhs, inverse, PLAIN)
        turning = cor[...]
        outs[1][...] = wet * (
            zold[...] + turning * mnow[...] - COURANT * metric * inner_diff(height, 0, line, columns)
        )
        outs[2][...] = mold[...] - COURANT * inner_diff(height, 1, lane, rows) - turning * znow[...]

        def across(v):
            return v[:, :columns] if columns <= rows else jnp.broadcast_to(v[:, :1], (1, columns))

        coarse, fine, reach = [None] * lats, [None] * lats, [None] * lats
        product = jnp.ones((1, rows), jnp.float32)
        for d in range(lats - 1, 0, -1):
            block = lax.rem(b_id + d, lats)
            product = product * own(4, block)
            coarse[d], fine[d], reach[d] = own(6, block) * product, own(7, block) * product, own(0, block) * product
        product = jnp.ones((1, rows), jnp.float32)
        for d in range(1, lats):
            block = lax.rem(b_id + d, lats)
            north = b_id + d < lats
            product = product * own(5, block)
            coarse[d] = jnp.where(north, own(8, block) * product, coarse[d])
            fine[d] = jnp.where(north, own(9, block) * product, fine[d])
            reach[d] = jnp.where(north, own(1, block) * product, reach[d])
        own_low = across(own(10, b_id)) * ends[0:1]
        own_high = across(own(11, b_id)) * ends[1:2]
        if turns:
            basis = [jnp.broadcast_to(columns_of[:, k : k + 1], (rows, columns)) for k in (2, 3)]
        else:
            basis = pieces(
                jnp.concatenate(
                    [
                        jnp.concatenate([yb_s, y_s] + [zero_row] * 6, axis=0),
                        jnp.concatenate([zero_row, zero_row, COURANT * first_row, -COURANT * last_row] + [zero_row] * 4, axis=0),
                    ],
                    axis=1,
                )
            )
            basis = jnp.concatenate([basis[k] for k in (0, 1, 2, 0, 1, 0)], axis=0).astype(jnp.bfloat16)
        full = jnp.ones((rows, rows), jnp.float32)
        lower = jnp.where(below, 1.0, 0.0)
        running = jnp.concatenate(
            [jnp.concatenate([lower, full], axis=0), jnp.concatenate([1.0 - lower, full], axis=0)], axis=1
        ).astype(jnp.bfloat16)

        for kind, ref in enumerate((recv_side, recv_next, lat_bytes)):
            pltpu.make_async_copy(ref, ref, send_sem.at[kind]).wait()
        return coarse[1:], fine[1:], reach[1:], own_low, own_high, basis, running, ay, ayb, y_s, yb_s

    coarse, fine, reach, own_low, own_high, basis, running, ay, ayb, y_s, yb_s = pl.run_scoped(
        early, pltpu.SemaphoreType.DMA((5,)), pltpu.SemaphoreType.DMA((3,))
    )
    coarse, fine, reach = [None, *coarse], [None, *fine], [None, *reach]

    def across(v):
        return v[:, :columns] if columns <= rows else jnp.broadcast_to(v[:, :1], (1, columns))

    zero_row = jnp.zeros((1, rows), jnp.float32)
    wet, metric = land[...].astype(jnp.float32), met[...]
    arrivals = ((1, recv_next), (0, recv_side), (2, lat_bytes))
    for kind, ref in arrivals:
        pltpu.make_async_copy(ref, ref, recv_sem.at[kind]).wait()

    low, high = own_low, own_high
    for d in range(1, lats):
        arrived = recv_lat[d - 1, 0:1] * across(coarse[d]) + recv_lat[d - 1, 1:2] * across(fine[d])
        north = b_id + d < lats
        high = high + jnp.where(north, arrived, 0.0)
        low = low + jnp.where(north, 0.0, arrived)
    south_height = jnp.where(b_id > 0, recv_lat[lats - 2, 2:3], 0.0)
    north_height = jnp.where(b_id < lats - 1, recv_lat[0, 2:3], 0.0)
    if turns:
        lat_at = lax.broadcasted_iota(jnp.int32, (rows, columns), 0)
        outside = jnp.where(
            lat_at == 0, COURANT * south_height, jnp.where(lat_at == rows - 1, -COURANT * north_height, 0.0)
        )
        height_term = jnp.transpose(basis[0] * low + basis[1] * high)
        velocity_term = jnp.transpose(outside)
    else:
        carried = pieces(
            jnp.concatenate([low, high, south_height, north_height, jnp.zeros((4, columns), jnp.float32)], axis=0)
        )
        carried = jnp.concatenate([carried[k] for k in (0, 0, 0, 1, 1, 2)], axis=0).astype(jnp.bfloat16)
        corrections = lax.dot_general(carried, basis, FIRST_WITH_FIRST, preferred_element_type=jnp.float32)
        height_term, velocity_term = corrections[:, :rows], corrections[:, rows:]

    lows, highs = [], []
    for side in (1, 0):
        flux = recv_next[side, 0:1]
        low, high = zero_row, zero_row
        for d in range(1, lats):
            arrived = recv_side[side, d - 1] * reach[d]
            north = b_id + d < lats
            high = high + jnp.where(north, arrived, 0.0)
            low = low + jnp.where(north, 0.0, arrived)
        lows.append(jnp.concatenate([flux * ay, low], axis=1))
        highs.append(jnp.concatenate([flux * ayb, high], axis=1))
    spare = jnp.zeros((4, 2 * rows), jnp.float32)
    edges = jnp.concatenate(pieces(jnp.concatenate(lows + highs + [spare], axis=0)), axis=0)
    edges = jnp.concatenate([edges, jnp.zeros((8, 2 * rows), jnp.float32)], axis=0).astype(jnp.bfloat16)
    edges = lax.dot_general(edges, running, PLAIN, preferred_element_type=jnp.float32)
    edges = edges[0:8] + edges[8:16] + edges[16:24]

    solved = outs[0][...] + height_term
    outs[0][...] = wet * solved
    outs[2][...] = wet * (outs[2][...] + velocity_term)
    for k, (at, side, sign) in enumerate(((0, 1, COURANT), (columns - 1, 0, -COURANT))):
        edge = pl.ds(at, 1)
        outs[0][edge, :] = wet[at : at + 1] * (
            solved[at : at + 1] + edges[k : k + 1, :rows] * yb_s + edges[2 + k : 3 + k, rows:] * y_s
        )
        outs[1][edge, :] = outs[1][edge, :] + wet[at : at + 1] * (sign * metric * recv_next[side, 1:2])


def store_kernel(*refs):
    def move(sem):
        stores = [pltpu.make_async_copy(refs[k], refs[3 + k], sem.at[k]) for k in range(3)]
        for store in stores:
            store.start()
        for store in stores:
            store.wait()

    pl.run_scoped(move, pltpu.SemaphoreType.DMA((3,)))


def per_device(lons, lats, *args):
    args = list(args)
    columns, rows = args[0].shape
    sources = args[11].shape[0]
    padded = -(-lats // 8) * 8
    args[8] = args[8].reshape(1, rows)
    args[9] = args[9].reshape(1, rows)
    args[10] = args[10].reshape(lats, rows)
    for k in (11, 12, 13):
        args[k] = args[k].reshape(1, sources)
    out = pltpu.VMEM((columns, rows), jnp.float32)
    others = lats - 1
    results = pl.pallas_call(
        functools.partial(kernel, lons, lats),
        out_shape=(out, out, out),
        in_specs=[pl.BlockSpec(memory_space=pl.ANY)] * 14,
        out_specs=(pl.BlockSpec(memory_space=pltpu.VMEM),) * 3,
        scratch_shapes=[
            pltpu.VMEM((8, columns, rows), jnp.float32),
            pltpu.VMEM((columns, rows), jnp.int32),
            pltpu.VMEM((2, 1, rows), jnp.float32),
            pltpu.VMEM((padded, rows), jnp.float32),
            pltpu.VMEM((1, sources), jnp.int32),
            pltpu.VMEM((1, sources), jnp.int32),
            pltpu.VMEM((3, 1, sources), jnp.float32),
            pltpu.VMEM((12, padded, rows), jnp.float32),
            pltpu.VMEM((8, padded, rows), jnp.float32),
            pltpu.VMEM((2, 4, columns), jnp.float32),
            pltpu.VMEM((2, 1, rows), jnp.float32),
            pltpu.VMEM((2, 2, rows), jnp.float32),
            pltpu.VMEM((others, 4, columns), jnp.float32),
            pltpu.VMEM((2, others, 1, rows), jnp.float32),
            pltpu.VMEM((2, 2, rows), jnp.float32),
            pltpu.SemaphoreType.DMA((3,)),
            pltpu.VMEM((2, 4, rows), jnp.float32),
            pltpu.VMEM((2, 1, rows), jnp.int32),
        ],
        compiler_params=pltpu.CompilerParams(collective_id=0, has_side_effects=True),
    )(*args)
    return pl.pallas_call(
        store_kernel,
        out_shape=(jax.ShapeDtypeStruct((columns, rows), jnp.float32),) * 3,
        in_specs=[pl.BlockSpec(memory_space=pltpu.VMEM)] * 3,
        out_specs=(pl.BlockSpec(memory_space=pl.ANY),) * 3,
    )(*[pltpu.with_memory_space_constraint(r, pltpu.VMEM) for r in results])


def solution(mesh):
    field = P("lon", "lat")
    placed = (field,) * 8 + (P("lat"),) * 2 + (P(),) * 4
    return jax.shard_map(
        functools.partial(per_device, mesh.shape["lon"], mesh.shape["lat"]),
        mesh=mesh,
        in_specs=placed,
        out_specs=(field,) * 3,
        check_vma=False,
    )
```

```python
import functools

import jax
import jax.numpy as jnp
from jax import lax
from jax.experimental import pallas as pl
from jax.experimental.pallas import tpu as pltpu
from jax.sharding import PartitionSpec as P

COURANT = 0.25
MESH = pl.DeviceIdType.MESH
HIGHEST = lax.Precision.HIGHEST
LAST_WITH_LAST = (((1,), (1,)), ((), ()))
FIRST_WITH_FIRST = (((0,), (0,)), ((), ()))
PLAIN = (((1,), (0,)), ((), ()))
WINDOW = 16
STRIDES = 8


def exact_dot(left, right, dims):
    return lax.dot_general(left, right, dims, precision=HIGHEST, preferred_element_type=jnp.float32)


def pieces(value):
    found = []
    for _ in range(3):
        piece = value.astype(jnp.bfloat16).astype(jnp.float32)
        found.append(piece)
        value = value - piece
    return found


def line_scan(a, lane, upward):
    rows = a.shape[1]
    one, zero = jnp.ones_like(a), jnp.zeros_like(a)

    def behind(v, amount):
        return pltpu.roll(v, amount if upward else rows - amount, 1)

    def inside(amount):
        return lane >= amount if upward else lane < rows - amount

    window = min(WINDOW, rows)
    m = [one, zero, zero, one]
    for i in range(window - 1, -1, -1):
        step = behind(a, i) if i else a
        keep = inside(i)
        for x, y in ((0, 2), (1, 3)):
            total = m[x] + m[y]
            grown = m[x] + step * total
            m[x] = jnp.where(keep, grown, m[x]) if i else grown
            m[y] = jnp.where(keep, total, m[y]) if i else total
    unit = (1.0, 0.0, 0.0, 1.0)
    while window < rows:
        count = min(STRIDES, rows // window)
        terms = [m]
        for i in range(1, count):
            keep = inside(i * window)
            terms.append([jnp.where(keep, behind(v, i * window), u) for v, u in zip(m, unit)])
        while len(terms) > 1:
            joined = []
            for p, q in zip(terms[0::2], terms[1::2]):
                joined.append(
                    [
                        p[0] * q[0] + p[1] * q[2],
                        p[0] * q[1] + p[1] * q[3],
                        p[2] * q[0] + p[3] * q[2],
                        p[2] * q[1] + p[3] * q[3],
                    ]
                )
            terms = joined + terms[2 * len(joined) :]
        m = terms[0]
        window *= count
    return m


def line_factors(a, up, down, before, after, blocks):
    padded, rows = a.shape
    one = jnp.ones_like(a)

    def carried(m, edge, order):
        m = [jnp.broadcast_to(v[:, edge : edge + 1], (padded, rows)) for v in m]
        x, y = one[:1], jnp.zeros_like(one[:1])
        xs, ys, shrink = {}, {}, {}
        for c in order:
            xs[c], ys[c] = x, y
            nx = m[0][c : c + 1] * x + m[1][c : c + 1] * y
            ny = m[2][c : c + 1] * x + m[3][c : c + 1] * y
            ratio = 1.0 / (nx + ny)
            shrink[c] = ratio
            x, y = nx * ratio, ny * ratio
        spare = [one[:1]] * (padded - blocks)
        return [jnp.concatenate([t[c] for c in range(blocks)] + spare, axis=0) for t in (xs, ys, shrink)]

    x_in, y_in, shrink_up = carried(up, rows - 1, range(blocks))
    xb_in, yb_in, shrink_down = carried(down, 0, range(blocks - 1, -1, -1))
    x = up[0] * x_in + up[1] * y_in
    y = up[2] * x_in + up[3] * y_in
    yb = down[2] * xb_in + down[3] * yb_in
    end = lambda v: jnp.broadcast_to(v[:, rows - 1 :], (padded, rows))
    scale = 1.0 / (end(x) + end(y) * xb_in)
    return (
        a * y,
        a * yb,
        y * scale,
        yb * scale,
        shrink_up,
        shrink_down,
        x_in,
        y_in,
        xb_in,
        yb_in,
        -before * y_in,
        after * yb_in,
    )


def kernel(lons, lats, *refs):
    ins, outs, refs = refs[:14], refs[14:17], refs[17:]
    (
        fields,
        land,
        pair,
        wgt,
        slon,
        slat,
        amp,
        factors,
        starts,
        send_lat,
        send_side,
        send_next,
        recv_lat,
        recv_side,
        recv_next,
        recv_sem,
        rim,
        rim_land,
    ) = refs
    a_id = lax.axis_index("lon")
    b_id = lax.axis_index("lat")
    sides = (lax.rem(a_id + lons - 1, lons), lax.rem(a_id + 1, lons))
    znow, depth, hnow, mnow, hold, zold, mold = (fields.at[k] for k in range(7))
    met, cor, samp = pair.at[0], pair.at[1], amp.at[0]
    columns, rows = land.shape
    trims = lats >= 4 and lats % 2 == 0
    lat_bytes = recv_lat.at[pl.ds(0, lats // 2)] if trims else recv_lat

    def part(k):
        return pl.ds(0, (3 if k in (1, lats - 1) else 2) if trims else 4)

    turns = columns % 128 == 0 and rows % 128 == 0
    padded = wgt.shape[0]

    def early(load_sem, send_sem):
        barrier = pltpu.get_barrier_semaphore()

        def load(group, number, to, at=None):
            source = ins[number] if at is None else ins[number].at[at]
            pltpu.make_async_copy(source, to, load_sem.at[group]).start()

        def loaded(group, ref):
            pltpu.make_async_copy(ref, ref, load_sem.at[group]).wait()

        for k, at in enumerate((0, columns - 1)):
            row = pl.ds(at, 1)
            load(0, 3, rim.at[k, pl.ds(0, 1)], row)
            load(0, 6, rim.at[k, pl.ds(1, 1)], row)
            load(0, 7, rim_land.at[k], row)
            load(0, 1, rim.at[k, pl.ds(2, 1)], row)
        load(1, 8, met)
        load(1, 9, cor)
        load(2, 10, wgt.at[pl.ds(0, lats)])
        load(4, 11, slon)
        load(4, 12, slat)
        load(4, 13, samp)
        south_half = 2 * b_id < lats
        for k in range(lats - 1):
            down, up_row = lats - 1 - k, k
            down = down - (down <= b_id).astype(jnp.int32)
            up_row = up_row + (up_row >= b_id).astype(jnp.int32)
            other = jnp.where(south_half, down, up_row)
            for column in (*sides, a_id):
                pl.semaphore_signal(barrier, inc=1, device_id=(column, other), device_id_type=MESH)
            if k == 0:
                for side in sides:
                    pl.semaphore_signal(barrier, inc=1, device_id=(side, b_id), device_id_type=MESH)
        for number, slot in ((3, znow), (6, depth), (7, land), (5, mnow), (0, hold), (1, hnow), (2, zold), (4, mold)):
            load(3, number, slot)

        loaded(0, rim)
        loaded(1, pair)
        scaled_metric = COURANT * met[...]
        for side, sign in enumerate((-1.0, 1.0)):
            flux = rim[side, 1:2] * rim_land[side].astype(jnp.float32) * rim[side, 0:1]
            flux = sign * scaled_metric * flux
            send_side[side] = flux
            send_next[side] = jnp.concatenate([flux, rim[side, 2:3]], axis=0)

        def remote(src, dst, kind, column, row):
            return pltpu.make_async_remote_copy(
                src_ref=src,
                dst_ref=dst,
                send_sem=send_sem.at[kind],
                recv_sem=recv_sem.at[kind],
                device_id=(column, row),
                device_id_type=MESH,
            )

        def send_moments(k):
            remote(
                send_lat.at[jnp.where(b_id + k < lats, 0, 1), part(k)],
                recv_lat.at[lats - k - 1, part(k)],
                2,
                a_id,
                lax.rem(b_id + k, lats),
            ).start()

        def greet_and_send(moments_too):
            pl.semaphore_wait(barrier, 3 * lats - 1)
            if moments_too:
                send_moments(1)
            for k in range(1, lats):
                row = k - 1 + (b_id <= k - 1).astype(jnp.int32)
                slot = lats - 2 - lax.rem(row - b_id + lats - 1, lats)
                for side in (1, 0):
                    remote(send_side.at[side], recv_side.at[side, slot], 0, sides[side], row).start()
                if k == 1:
                    for side in (1, 0):
                        remote(send_next.at[side], recv_next.at[side], 1, sides[side], b_id).start()
            if moments_too:
                for k in range(2, lats):
                    send_moments(k)

        far = jnp.logical_and(2 * b_id >= lats, a_id > 1)
        pl.when(far)(lambda: greet_and_send(False))

        loaded(2, wgt.at[pl.ds(0, lats)])
        loaded(4, amp)
        sources = slon.shape[1]
        east_cell = lax.broadcasted_iota(jnp.int32, (columns, sources), 0) + a_id * columns
        north_cell = lax.broadcasted_iota(jnp.int32, (rows, sources), 0) + b_id * rows
        hit_east = east_cell == slon[...]
        hit_north = jnp.where(north_cell == slat[...], 1.0, 0.0).astype(jnp.bfloat16)
        added = [
            lax.dot_general(
                jnp.where(hit_east, piece, 0.0).astype(jnp.bfloat16),
                hit_north,
                LAST_WITH_LAST,
                preferred_element_type=jnp.float32,
            )
            for piece in pieces(samp[...])
        ]
        added = added[0] + added[1] + added[2]
        weight = wgt[...]
        if padded > lats:
            row_id = lax.broadcasted_iota(jnp.int32, (padded, rows), 0)
            weight = jnp.where(row_id < lats, weight, 1.0)
        a = 1.0 / weight
        lane_of = lax.broadcasted_iota(jnp.int32, (padded, rows), 1)
        first_lane, last_lane = lane_of == 0, lane_of == rows - 1
        before = COURANT * pltpu.roll(jnp.broadcast_to(a[:, rows - 1 :], (padded, rows)), 1, 0)
        after = COURANT * pltpu.roll(jnp.broadcast_to(a[:, :1], (padded, rows)), padded - 1, 0)
        up = line_scan(a, lane_of, True)
        down = line_scan(a, lane_of, False)
        zeros = jnp.zeros_like(a)
        at_last = lambda v: jnp.where(last_lane, v, zeros)
        at_first = lambda v: jnp.where(first_lane, v, zeros)
        for k, value in enumerate(
            (
                a * up[2],
                a * up[3],
                a * down[2],
                a * down[3],
                at_last((up[0] + up[2]) * after),
                at_last((up[1] + up[3]) * after) - at_first(before),
                -at_first((down[0] + down[2]) * before),
                at_last(after) - at_first((down[1] + down[3]) * before),
            )
        ):
            starts[k] = value

        loaded(3, fields)
        wet = land[...].astype(jnp.float32)
        wet_depth = depth[...] * wet
        flux_east = wet_depth * znow[...]
        flux_north = wet_depth * mnow[...]
        metric = met[...]
        line = lax.broadcasted_iota(jnp.int32, (columns, rows), 0)
        lane = lax.broadcasted_iota(jnp.int32, (columns, rows), 1)

        def inner_diff(v, axis, position, size):
            ahead = jnp.where(position == size - 1, 0.0, pltpu.roll(v, size - 1, axis))
            behind = jnp.where(position == 0, 0.0, pltpu.roll(v, 1, axis))
            return ahead - behind

        rhs = added + hold[...] - COURANT * (
            metric * inner_diff(flux_east, 0, line, columns) + inner_diff(flux_north, 1, lane, rows)
        )
        height = hnow[...]
        row_lane = lax.broadcasted_iota(jnp.int32, (1, rows), 1)
        first_row = jnp.where(row_lane == 0, 1.0, 0.0)
        last_row = jnp.where(row_lane == rows - 1, 1.0, 0.0)
        zero_row = jnp.zeros((1, rows), jnp.float32)
        outer = exact_dot(
            jnp.concatenate([zero_row, zero_row, last_row, zero_row] + [zero_row] * 2 + [first_row, zero_row], axis=0),
            height,
            LAST_WITH_LAST,
        )
        def start(k):
            return starts[k, pl.ds(b_id, 1), :]

        def laid(k):
            return jnp.concatenate(
                [start(k), start(k + 1), zero_row, zero_row, start(k + 2), start(k + 3), zero_row, zero_row], axis=0
            )

        moments = outer + exact_dot(
            jnp.concatenate([laid(0), laid(4)], axis=1),
            jnp.concatenate([rhs, flux_north], axis=1),
            LAST_WITH_LAST,
        )
        send_lat[0] = moments[0:4]
        send_lat[1] = moments[4:8]
        @pl.when(jnp.logical_not(far))
        def _():
            greet_and_send(True)

        @pl.when(far)
        def _():
            for k in range(1, lats):
                send_moments(k)

        ends = exact_dot(
            jnp.concatenate([first_row, last_row] + [zero_row] * 6, axis=0), flux_north, LAST_WITH_LAST
        )

        for k, value in enumerate(line_factors(a, up, down, before, after, lats)):
            factors[k] = value

        def own(k, block):
            return factors[k, pl.ds(block, 1), :]

        ay, ayb, y_s, yb_s = [own(k, b_id) for k in range(4)]
        columns_of = jnp.transpose(jnp.concatenate([ay, ayb, yb_s, y_s] + [zero_row] * 4, axis=0))
        source_lat = lax.broadcasted_iota(jnp.int32, (rows, rows), 0)
        target_lat = lax.broadcasted_iota(jnp.int32, (rows, rows), 1)
        below = source_lat <= target_lat
        inverse = jnp.where(below, columns_of[:, 0:1] * yb_s, columns_of[:, 1:2] * y_s)
        outs[0][...] = exact_dot(rhs, inverse, PLAIN)
        turning = cor[...]
        outs[1][...] = wet * (
            zold[...] + turning * mnow[...] - COURANT * metric * inner_diff(height, 0, line, columns)
        )
        outs[2][...] = mold[...] - COURANT * inner_diff(height, 1, lane, rows) - turning * znow[...]

        def across(v):
            return v[:, :columns] if columns <= rows else jnp.broadcast_to(v[:, :1], (1, columns))

        coarse, fine, reach = [None] * lats, [None] * lats, [None] * lats
        product = jnp.ones((1, rows), jnp.float32)
        for d in range(lats - 1, 0, -1):
            block = lax.rem(b_id + d, lats)
            product = product * own(4, block)
            coarse[d], fine[d], reach[d] = own(6, block) * product, own(7, block) * product, own(0, block) * product
        product = jnp.ones((1, rows), jnp.float32)
        for d in range(1, lats):
            block = lax.rem(b_id + d, lats)
            north = b_id + d < lats
            product = product * own(5, block)
            coarse[d] = jnp.where(north, own(8, block) * product, coarse[d])
            fine[d] = jnp.where(north, own(9, block) * product, fine[d])
            reach[d] = jnp.where(north, own(1, block) * product, reach[d])
        own_low = across(own(10, b_id)) * ends[0:1]
        own_high = across(own(11, b_id)) * ends[1:2]
        if turns:
            basis = [jnp.broadcast_to(columns_of[:, k : k + 1], (rows, columns)) for k in (2, 3)]
        else:
            basis = pieces(
                jnp.concatenate(
                    [
                        jnp.concatenate([yb_s, y_s] + [zero_row] * 6, axis=0),
                        jnp.concatenate([zero_row, zero_row, COURANT * first_row, -COURANT * last_row] + [zero_row] * 4, axis=0),
                    ],
                    axis=1,
                )
            )
            basis = jnp.concatenate([basis[k] for k in (0, 1, 2, 0, 1, 0)], axis=0).astype(jnp.bfloat16)
        full = jnp.ones((rows, rows), jnp.float32)
        lower = jnp.where(below, 1.0, 0.0)
        running = jnp.concatenate(
            [jnp.concatenate([lower, full], axis=0), jnp.concatenate([1.0 - lower, full], axis=0)], axis=1
        ).astype(jnp.bfloat16)

        for kind, ref in enumerate((recv_side, recv_next, lat_bytes)):
            pltpu.make_async_copy(ref, ref, send_sem.at[kind]).wait()
        return coarse[1:], fine[1:], reach[1:], own_low, own_high, basis, running, ay, ayb, y_s, yb_s

    coarse, fine, reach, own_low, own_high, basis, running, ay, ayb, y_s, yb_s = pl.run_scoped(
        early, pltpu.SemaphoreType.DMA((5,)), pltpu.SemaphoreType.DMA((3,))
    )
    coarse, fine, reach = [None, *coarse], [None, *fine], [None, *reach]

    def across(v):
        return v[:, :columns] if columns <= rows else jnp.broadcast_to(v[:, :1], (1, columns))

    zero_row = jnp.zeros((1, rows), jnp.float32)
    wet, metric = land[...].astype(jnp.float32), met[...]
    arrivals = ((1, recv_next), (0, recv_side), (2, lat_bytes))
    for kind, ref in arrivals:
        pltpu.make_async_copy(ref, ref, recv_sem.at[kind]).wait()

    low, high = own_low, own_high
    for d in range(1, lats):
        arrived = recv_lat[d - 1, 0:1] * across(coarse[d]) + recv_lat[d - 1, 1:2] * across(fine[d])
        north = b_id + d < lats
        high = high + jnp.where(north, arrived, 0.0)
        low = low + jnp.where(north, 0.0, arrived)
    south_height = jnp.where(b_id > 0, recv_lat[lats - 2, 2:3], 0.0)
    north_height = jnp.where(b_id < lats - 1, recv_lat[0, 2:3], 0.0)
    if turns:
        lat_at = lax.broadcasted_iota(jnp.int32, (rows, columns), 0)
        outside = jnp.where(
            lat_at == 0, COURANT * south_height, jnp.where(lat_at == rows - 1, -COURANT * north_height, 0.0)
        )
        height_term = jnp.transpose(basis[0] * low + basis[1] * high)
        velocity_term = jnp.transpose(outside)
    else:
        carried = pieces(
            jnp.concatenate([low, high, south_height, north_height, jnp.zeros((4, columns), jnp.float32)], axis=0)
        )
        carried = jnp.concatenate([carried[k] for k in (0, 0, 0, 1, 1, 2)], axis=0).astype(jnp.bfloat16)
        corrections = lax.dot_general(carried, basis, FIRST_WITH_FIRST, preferred_element_type=jnp.float32)
        height_term, velocity_term = corrections[:, :rows], corrections[:, rows:]

    lows, highs = [], []
    for side in (1, 0):
        flux = recv_next[side, 0:1]
        low, high = zero_row, zero_row
        for d in range(1, lats):
            arrived = recv_side[side, d - 1] * reach[d]
            north = b_id + d < lats
            high = high + jnp.where(north, arrived, 0.0)
            low = low + jnp.where(north, 0.0, arrived)
        lows.append(jnp.concatenate([flux * ay, low], axis=1))
        highs.append(jnp.concatenate([flux * ayb, high], axis=1))
    spare = jnp.zeros((4, 2 * rows), jnp.float32)
    edges = jnp.concatenate(pieces(jnp.concatenate(lows + highs + [spare], axis=0)), axis=0)
    edges = jnp.concatenate([edges, jnp.zeros((8, 2 * rows), jnp.float32)], axis=0).astype(jnp.bfloat16)
    edges = lax.dot_general(edges, running, PLAIN, preferred_element_type=jnp.float32)
    edges = edges[0:8] + edges[8:16] + edges[16:24]

    solved = outs[0][...] + height_term
    outs[0][...] = wet * solved
    outs[2][...] = wet * (outs[2][...] + velocity_term)
    for k, (at, side, sign) in enumerate(((0, 1, COURANT), (columns - 1, 0, -COURANT))):
        edge = pl.ds(at, 1)
        outs[0][edge, :] = wet[at : at + 1] * (
            solved[at : at + 1] + edges[k : k + 1, :rows] * yb_s + edges[2 + k : 3 + k, rows:] * y_s
        )
        outs[1][edge, :] = outs[1][edge, :] + wet[at : at + 1] * (sign * metric * recv_next[side, 1:2])


def store_kernel(*refs):
    def move(sem):
        stores = [pltpu.make_async_copy(refs[k], refs[3 + k], sem.at[k]) for k in range(3)]
        for store in stores:
            store.start()
        for store in stores:
            store.wait()

    pl.run_scoped(move, pltpu.SemaphoreType.DMA((3,)))


def per_device(lons, lats, *args):
    args = list(args)
    columns, rows = args[0].shape
    sources = args[11].shape[0]
    padded = -(-lats // 8) * 8
    args[8] = args[8].reshape(1, rows)
    args[9] = args[9].reshape(1, rows)
    args[10] = args[10].reshape(lats, rows)
    for k in (11, 12, 13):
        args[k] = args[k].reshape(1, sources)
    out = pltpu.VMEM((columns, rows), jnp.float32)
    others = lats - 1
    results = pl.pallas_call(
        functools.partial(kernel, lons, lats),
        out_shape=(out, out, out),
        in_specs=[pl.BlockSpec(memory_space=pl.ANY)] * 14,
        out_specs=(pl.BlockSpec(memory_space=pltpu.VMEM),) * 3,
        scratch_shapes=[
            pltpu.VMEM((8, columns, rows), jnp.float32),
            pltpu.VMEM((columns, rows), jnp.int32),
            pltpu.VMEM((2, 1, rows), jnp.float32),
            pltpu.VMEM((padded, rows), jnp.float32),
            pltpu.VMEM((1, sources), jnp.int32),
            pltpu.VMEM((1, sources), jnp.int32),
            pltpu.VMEM((3, 1, sources), jnp.float32),
            pltpu.VMEM((12, padded, rows), jnp.float32),
            pltpu.VMEM((8, padded, rows), jnp.float32),
            pltpu.VMEM((2, 4, columns), jnp.float32),
            pltpu.VMEM((2, 1, rows), jnp.float32),
            pltpu.VMEM((2, 2, rows), jnp.float32),
            pltpu.VMEM((others, 4, columns), jnp.float32),
            pltpu.VMEM((2, others, 1, rows), jnp.float32),
            pltpu.VMEM((2, 2, rows), jnp.float32),
            pltpu.SemaphoreType.DMA((3,)),
            pltpu.VMEM((2, 4, rows), jnp.float32),
            pltpu.VMEM((2, 1, rows), jnp.int32),
        ],
        compiler_params=pltpu.CompilerParams(collective_id=0, has_side_effects=True),
    )(*args)
    return pl.pallas_call(
        store_kernel,
        out_shape=(jax.ShapeDtypeStruct((columns, rows), jnp.float32),) * 3,
        in_specs=[pl.BlockSpec(memory_space=pltpu.VMEM)] * 3,
        out_specs=(pl.BlockSpec(memory_space=pl.ANY),) * 3,
    )(*[pltpu.with_memory_space_constraint(r, pltpu.VMEM) for r in results])


def solution(mesh):
    field = P("lon", "lat")
    placed = (field,) * 8 + (P("lat"),) * 2 + (P(),) * 4
    return jax.shard_map(
        functools.partial(per_device, mesh.shape["lon"], mesh.shape["lat"]),
        mesh=mesh,
        in_specs=placed,
        out_specs=(field,) * 3,
        check_vma=False,
    )
```
